32 devices in a mesh: row: 8 (over y, x, core), col: 4 (over z).
Axes of the slice: x: 2, y: 2, z: 4, core: 2. Of those that a mesh axis runs over, the one named last changes fastest.
Arguments:
- features: bfloat16 [16384, 256], P(('row', 'col')), may hold values from -1 to 3
- in_degree: int32 [16384], P(('row', 'col')), may hold values from 512 to 2047
- tile_index: int32 [8192, 2], P(('row', 'col')), may hold values from 0 to 31, as said below
- tile_count: int32 [32], P(('row', 'col')), may hold values from 1 to 256, as said below
- adjacency_tiles: bfloat16 [8192, 128, 128], P(('row', 'col')), may hold values from 0 to 1, as said below
- projection: bfloat16 [512, 256], replicated, may hold values from -0.25 to 0.25
- out_bias: float32 [256], replicated, may hold values from -3 to 3
Outputs:
- hidden_out: bfloat16 [16384, 256], P(('row', 'col'))
The draws below stay inside these ranges and needn't reach their ends.
Inputs may be any that keep to these rules, and one draw needn't show every extreme that they name: `tile_index`: column 0 is a local row block below 16, column 1 a local column block below 32, in every slot. `tile_count`: slots at or beyond the count hold tiles and indices that must be ignored; some device has all 256 slots live in every draw. `adjacency_tiles`: entries are 0 or 1.
All inputs are finite; a program needn't handle non-finite values.
Results may differ from the reference program's by a relative error of at most 0.0034.
Values may be sent and summed in bfloat16 or wider, within the bound.
A program may use at most 128 MiB of HBM per device.

```python
import jax
import jax.numpy as jnp
from jax import lax

F = 256
H = 256
TILE = 128
VB_DEV = 4
MAX_TILES = 256
RB = 16
CB = 32
V = 16384
N_ROW = 8
N_COL = 4


def draw_tile_index(key, part):
    slots = N_ROW * N_COL * MAX_TILES
    row_part = jax.random.randint(jax.random.fold_in(key, 11), (slots,), 0, VB_DEV * N_COL)
    col_part = jax.random.randint(jax.random.fold_in(key, 12), (slots,), 0, VB_DEV * N_ROW)
    return jnp.stack([row_part, col_part], axis=1).astype(jnp.int32)


def draw_tile_count(key, part):
    devices = N_ROW * N_COL
    counts = jax.random.randint(jax.random.fold_in(key, 21), (devices,), max(1, MAX_TILES // 8), MAX_TILES + 1)
    fullest = jax.random.randint(jax.random.fold_in(key, 22), (), 0, devices)
    placed = jnp.arange(devices, dtype=jnp.int32) == fullest
    return jnp.where(placed, MAX_TILES, counts).astype(jnp.int32)


def draw_adjacency_tiles(key, part):
    shape = (N_ROW * N_COL * MAX_TILES, TILE, TILE)
    uniform_draw = jax.random.uniform(jax.random.fold_in(key, 31), shape, jnp.float32)
    return jnp.where(uniform_draw < 0.25, 1.0, 0.0).astype(jnp.float32).astype(jnp.bfloat16)


def place_ends(drawn, own_key, low, largest):
    longest = drawn.shape.index(max(drawn.shape))
    spots = []
    for shift in (0, 1):
        where = [jax.random.randint(jax.random.fold_in(own_key, axis), (), 0, length) for axis, length in enumerate(drawn.shape)]
        where[longest] = (where[longest] + shift) % drawn.shape[longest]
        spots.append(tuple(where))
    return drawn.at[spots[0]].set(low).at[spots[1]].set(largest)


def shard_levels(own_key, extent, split, low, largest):
    def one(axis_at, parts):
        heights = jax.random.uniform(jax.random.fold_in(jax.random.fold_in(own_key, 6), axis_at), (parts,), jnp.float32, low / len(split), largest / len(split))
        return jnp.repeat(jnp.exp(heights), extent[axis_at] // parts).reshape((-1,) + (1,) * (len(extent) - axis_at - 1))

    level = one(*split[0])
    for cut in split[1:]:
        level = level * one(*cut)
    return level


def centred(key, dims, width, limit, held_as=jnp.bfloat16):
    array = jax.random.normal(key, dims, jnp.float32) * width
    return jnp.minimum(jnp.maximum(array, -limit), limit).astype(held_as)


def setup_inputs(seed: int = 0) -> dict:
    keys = jax.random.split(jax.random.key(seed), 8)
    features = jnp.clip(-1.0 + 4.0 * jax.random.uniform(keys[0], (V, F), jnp.float32) ** shard_levels(keys[0], (V, F), ((0, 32),), -0.2, 0.2), -1.0, 3.0).astype(jnp.bfloat16)
    in_degree = place_ends(jax.random.randint(keys[1], (V,), max(1, MAX_TILES * TILE // (VB_DEV * 16)), max(2, MAX_TILES * TILE // (VB_DEV * 4))), jax.random.fold_in(keys[1], 1), max(1, MAX_TILES * TILE // (VB_DEV * 16)), (max(2, MAX_TILES * TILE // (VB_DEV * 4))) - 1).astype(jnp.int32)
    tile_index = draw_tile_index(jax.random.fold_in(keys[7], 71), 0)
    tile_count = draw_tile_count(jax.random.fold_in(keys[7], 71), 0)
    adjacency_tiles = draw_adjacency_tiles(jax.random.fold_in(keys[7], 71), 0)
    projection = centred(keys[5], (2 * F, H), (2 * F) ** -0.5, 0.25)
    out_bias = centred(keys[6], (H,), 0.5, 3.0, jnp.float32)
    return {"features": features, "in_degree": in_degree, "tile_index": tile_index, "tile_count": tile_count, "adjacency_tiles": adjacency_tiles, "projection": projection, "out_bias": out_bias}


def device_partial(column_rows, slot_index, live_count, slot_tiles):
    blocks = column_rows.reshape(CB, TILE, F).astype(jnp.float32)[slot_index[:, 1]]
    alive = (jnp.arange(MAX_TILES, dtype=jnp.int32) < live_count).astype(jnp.float32)
    masked = slot_tiles.astype(jnp.float32) * alive[:, None, None]
    product = jnp.einsum("kij,kjf->kif", masked, blocks)
    summed = jax.ops.segment_sum(product, slot_index[:, 0], num_segments=RB)
    return summed.reshape(RB * TILE, F)


def reference(features, in_degree, tile_index, tile_count, adjacency_tiles, projection, out_bias):
    span = VB_DEV * TILE
    grouped = features.reshape(N_ROW, N_COL, span, F)

    def per_row(row_id):
        def per_col(running, col_id):
            column_rows = jnp.take(grouped, col_id, axis=1).reshape(N_ROW * span, F)
            device = row_id * N_COL + col_id
            slot_index = lax.dynamic_slice_in_dim(tile_index, device * MAX_TILES, MAX_TILES, 0)
            slot_tiles = lax.dynamic_slice_in_dim(adjacency_tiles, device * MAX_TILES, MAX_TILES, 0)
            live_count = tile_count[device]
            return running + device_partial(column_rows, slot_index, live_count, slot_tiles), None

        zeroed = jnp.zeros((RB * TILE, F), jnp.float32)
        summed, _ = lax.scan(per_col, zeroed, jnp.arange(N_COL, dtype=jnp.int32))
        return summed

    sums = lax.map(per_row, jnp.arange(N_ROW, dtype=jnp.int32)).reshape(V, F)
    neighbour_mean = (sums / in_degree[:, None].astype(jnp.float32)).astype(jnp.bfloat16)
    joined = jnp.concatenate([features, neighbour_mean], axis=1)
    mixed = jnp.dot(joined, projection, preferred_element_type=jnp.float32) + out_bias[None, :]
    return jnp.maximum(mixed, 0.0).astype(jnp.bfloat16)
```

```python
import functools

import jax
import jax.numpy as jnp
from jax import lax
from jax.experimental import pallas as pl
from jax.experimental.pallas import tpu as pltpu
from jax.sharding import PartitionSpec as P

BLK = 32
LANES = 128
CHUNKS = 16
PIECES = 2
UNROLL = 8
MERGE_LIMIT = 20 * 1024 * 1024
MESH = pl.DeviceIdType.MESH


def block_terms(running, col_blocks, index_block, tile_block, live_block):
    picked = col_blocks[index_block[:, 1]]
    kept = jnp.where(live_block[:, None, None], tile_block, jnp.zeros_like(tile_block))
    product = jnp.einsum("kij,kjf->kif", kept, picked, preferred_element_type=jnp.float32)
    flattened = product.reshape(product.shape[0], -1)
    return running.at[index_block[:, 0]].add(flattened)


def local_sparse(features, in_degree, tile_index, tile_count, adjacency_tiles, projection, out_bias):
    feat_width = features.shape[1]
    tile_size = adjacency_tiles.shape[1]
    slot_total = adjacency_tiles.shape[0]
    gathered = lax.all_gather(features, "row", axis=0, tiled=True)
    col_blocks = gathered.reshape(gathered.shape[0] // tile_size, tile_size, feat_width)
    row_blocks = features.shape[0] * lax.axis_size("col") // tile_size
    live_count = tile_count[0]
    zeroed = jnp.zeros((row_blocks, tile_size * feat_width), jnp.float32)

    def one_step(running, offset):
        index_block = lax.dynamic_slice_in_dim(tile_index, offset, BLK, 0)
        tile_block = lax.dynamic_slice_in_dim(adjacency_tiles, offset, BLK, 0)
        live_block = offset + jnp.arange(BLK, dtype=jnp.int32) < live_count
        return (block_terms(running, col_blocks, index_block, tile_block, live_block), None)

    summed, _ = lax.scan(one_step, zeroed, jnp.arange(0, slot_total, BLK, dtype=jnp.int32))
    partial_value = summed.reshape(row_blocks * tile_size, feat_width)
    own_sums = lax.psum_scatter(partial_value, "col", scatter_dimension=0, tiled=True)
    neighbour_mean = (own_sums / in_degree[:, None].astype(jnp.float32)).astype(jnp.bfloat16)
    joined = jnp.concatenate([features, neighbour_mean], axis=1)
    mixed = jnp.dot(joined, projection, preferred_element_type=jnp.float32) + out_bias[None, :]
    return jnp.maximum(mixed, 0.0).astype(jnp.bfloat16)


def slot_tables(place_ref, count, table_ref, row_blocks, positions):
    slots = place_ref.shape[1]
    chunks = slots // LANES
    slot_row = lax.broadcasted_iota(jnp.int32, (1, slots), 1)
    spot_row = place_ref[1:2, :] * row_blocks + place_ref[0:1, :]
    spot_row = jnp.where(slot_row < count, spot_row, positions)

    def lane(v, i):
        return v[:, i * LANES:(i + 1) * LANES]

    spot = jnp.concatenate(
        [jnp.transpose(jnp.broadcast_to(lane(spot_row, i), (LANES, LANES))) for i in range(chunks)], axis=0)
    slot = lax.broadcasted_iota(jnp.int32, (slots, LANES), 0)
    before = jnp.zeros((slots, LANES), jnp.float32)
    repeat = jnp.zeros((slots, LANES), jnp.float32)
    for i in range(chunks):
        equal = lane(spot_row, i) == spot
        earlier = lane(slot_row, i) < slot
        first = (lane(spot_row, i) < spot) | (equal & earlier)
        before = before + jnp.where(first, 1.0, 0.0)
        repeat = jnp.maximum(repeat, jnp.where(equal & earlier, 1.0, 0.0))
    rank = jnp.sum(before, axis=1, keepdims=True).astype(jnp.int32)
    keep = jnp.max(repeat, axis=1, keepdims=True)
    for i in range(chunks):
        hit = rank == lax.broadcasted_iota(jnp.int32, (slots, LANES), 1) + i * LANES
        order = jnp.sum(jnp.where(hit, slot, 0), axis=0, keepdims=True)
        again = jnp.sum(jnp.where(hit, keep, 0.0), axis=0, keepdims=True)
        table_ref[i:i + 1, :] = order
        table_ref[chunks + i:chunks + i + 1, :] = again.astype(jnp.int32)
    for i in range(positions // LANES):
        here = lax.broadcasted_iota(jnp.int32, (slots, LANES), 1) + i * LANES
        upto = jnp.sum(jnp.where(spot <= here, 1, 0), axis=0, keepdims=True)
        count_here = jnp.sum(jnp.where(spot == here, 1, 0), axis=0, keepdims=True)
        table_ref[2 * chunks + i:2 * chunks + i + 1, :] = jnp.where(count_here > 0, upto - 1, slots)


def fused_kernel(feat_ref, place_ref, count_ref, tiles_ref, degree_ref, proj_ref, bias_ref, out_ref,
                 stage, merged, table_v, table, gathered, acc, hidden, degree_col, send, relayed, landed,
                 tile_sem, table_sem, ag_send, ag_recv, send_sem, relay_sem, land_sem):
    seg, width = feat_ref.shape
    slots, tile, _ = stage.shape
    halves = width // LANES
    blocks = seg // tile
    row_blocks = acc.shape[1] // tile
    positions = blocks * gathered.shape[1] * row_blocks
    half_rows = seg // 2
    piece_rows = seg // PIECES
    per = slots // CHUNKS
    r = lax.axis_index("row")
    c = lax.axis_index("col")
    near = c ^ 1
    upper = c < 2
    outer = (c == 0) | (c == 3)
    dests = (jnp.where(upper, 3, 0), jnp.where(upper, 2, 1), near, c)

    def load(i):
        part = pl.ds(i * per, per)
        return pltpu.make_async_copy(tiles_ref.at[part], stage.at[part], tile_sem.at[i])

    for i in range(CHUNKS):
        load(i).start()

    barrier = pltpu.get_barrier_semaphore()

    def greet(row, col):
        pl.semaphore_signal(barrier, inc=1, device_id=(row, col), device_id_type=MESH)

    for m in (1, 2, 4):
        greet(r ^ m, c)
    greet(r, near)
    greet(r, c ^ 2)

    @pl.when(jnp.logical_not(outer))
    def _():
        greet(r, c ^ 3)

    pl.semaphore_wait(barrier, jnp.where(outer, 5, 6))

    OWN_SIB, OWN_XA, OWN_XB, OWN_YB, OWN_YA, FWD_Y, FWD_X, SIB_X, SIB_Y, SIB_D = range(10)
    first_rows, last_rows = pl.ds(0, half_rows), pl.ds(half_rows, half_rows)
    whole = pl.ds(0, seg)
    gather_plan = {
        OWN_SIB: (0, whole, 1), OWN_XA: (0, first_rows, 2), OWN_XB: (0, last_rows, 2),
        OWN_YB: (0, last_rows, 4), OWN_YA: (0, first_rows, 4),
        FWD_Y: (2, first_rows, 4), FWD_X: (4, last_rows, 2),
        SIB_X: (2, whole, 1), SIB_Y: (4, whole, 1), SIB_D: (6, whole, 1),
    }

    def lanes(h):
        return pl.ds(h * LANES, LANES)

    def gather_copy(h, j):
        flip, rows, step = gather_plan[j]
        owner = r ^ flip
        src = feat_ref.at[rows, lanes(h)] if flip == 0 else gathered.at[h, owner, rows, :]
        return pltpu.make_async_remote_copy(
            src_ref=src, dst_ref=gathered.at[h, owner, rows, :],
            send_sem=ag_send.at[h, j], recv_sem=ag_recv.at[h, j],
            device_id=(r ^ step, c), device_id_type=MESH)

    def gather_own(h):
        for j in (OWN_XA, OWN_YB, OWN_SIB, OWN_XB, OWN_YA):
            gather_copy(h, j).start()

    def forward(h):
        gather_copy(h, OWN_XA).wait_recv()
        gather_copy(h, FWD_Y).start()
        gather_copy(h, OWN_YB).wait_recv()
        gather_copy(h, FWD_X).start()

    def share_near(h):
        gather_copy(h, OWN_XB).wait_recv()
        gather_copy(h, SIB_X).start()
        gather_copy(h, OWN_YA).wait_recv()
        gather_copy(h, SIB_Y).start()

    def share_far(h):
        gather_copy(h, FWD_Y).wait_recv()
        gather_copy(h, FWD_X).wait_recv()
        gather_copy(h, SIB_D).start()

    def block_of(h, flip):
        return feat_ref[:, lanes(h)] if flip == 0 else gathered[h, r ^ flip]

    def product(h, flips, dest):
        columns = []
        for flip in flips:
            base = (r ^ flip) * (blocks * row_blocks)
            line = 2 * (slots // LANES) + base // LANES
            spot = base % LANES + dest * blocks
            columns += [(line, spot + k * row_blocks) for k in range(blocks)]
        left = jnp.concatenate(
            [jnp.concatenate([merged[table[line, spot + b]] for line, spot in columns], axis=1)
             for b in range(blocks)], axis=0)
        right = jnp.concatenate([block_of(h, flip) for flip in flips], axis=0)
        return jnp.dot(left, right, preferred_element_type=jnp.float32)

    def segment(dest):
        return pl.ds(pl.multiple_of(dest * seg, seg), seg)

    def add_pair(h, flips, first):
        @pl.loop(0, 3)
        def _(i):
            dest = jnp.where(i == 0, dests[0], jnp.where(i == 1, dests[1], dests[2]))
            if first:
                acc[h, segment(dest), :] = product(h, flips, dest)
            else:
                acc[h, segment(dest), :] += product(h, flips, dest)

    def piece(q):
        return pl.ds(q * piece_rows, piece_rows)

    def term(h, dest, q):
        return acc[h, pl.ds(pl.multiple_of(dest * seg + q * piece_rows, piece_rows), piece_rows), :]

    def relay_copy(h, i, q):
        return pltpu.make_async_remote_copy(
            src_ref=send.at[h, i, piece(q), :], dst_ref=relayed.at[h, i, piece(q), :],
            send_sem=send_sem.at[h, i, q], recv_sem=relay_sem.at[h, i, q],
            device_id=(r, near), device_id_type=MESH)

    def near_copy(h, q):
        return pltpu.make_async_remote_copy(
            src_ref=send.at[h, 2, piece(q), :], dst_ref=landed.at[h, 0, piece(q), :],
            send_sem=send_sem.at[h, 2, q], recv_sem=land_sem.at[h, 0, q],
            device_id=(r, near), device_id_type=MESH)

    def far_copy(h, i, q):
        return pltpu.make_async_remote_copy(
            src_ref=send.at[h, i, piece(q), :], dst_ref=landed.at[h, 1, piece(q), :],
            send_sem=send_sem.at[h, i, q], recv_sem=land_sem.at[h, 1, q],
            device_id=(r, dests[i]), device_id_type=MESH)

    def send_sum(h, i):
        if i == 2:
            for q in range(PIECES):
                send[h, i, piece(q), :] = term(h, dests[i], q).astype(send.dtype)
                near_copy(h, q).start()
        else:
            @pl.when(outer)
            def _():
                for q in range(PIECES):
                    send[h, i, piece(q), :] = term(h, dests[i], q).astype(send.dtype)
                    relay_copy(h, i, q).start()

    def relay_sum(h, i):
        @pl.when(jnp.logical_not(outer))
        def _():
            for q in range(PIECES):
                relay_copy(h, i, q).wait_recv()
                arrived = relayed[h, i, piece(q), :].astype(jnp.float32)
                send[h, i, piece(q), :] = (term(h, dests[i], q) + arrived).astype(send.dtype)
                far_copy(h, i, q).start()

    def last_pair(h, i):
        acc[h, segment(dests[i]), :] += product(h, (6, 7), dests[i])
        send_sum(h, i)

    def own_segment(h):
        total = product(h, (0, 1), c)
        for flips in ((2, 3), (4, 5), (6, 7)):
            total = total + product(h, flips, c)
        acc[h, segment(c), :] = total

    def finish(h):
        for q in range(PIECES):
            near_copy(h, q).wait_recv()
            far_copy(h, 0, q).wait_recv()
            total = (term(h, c, q) + landed[h, 0, piece(q), :].astype(jnp.float32)
                     + landed[h, 1, piece(q), :].astype(jnp.float32))
            mean = (total / degree_col[piece(q), :]).astype(jnp.bfloat16)
            mixed = hidden[piece(q), :] + jnp.dot(
                mean, proj_ref[width + h * LANES:width + (h + 1) * LANES, :],
                preferred_element_type=jnp.float32)
            if h + 1 < halves:
                hidden[piece(q), :] = mixed
            else:
                out_ref[piece(q), :] = jnp.maximum(mixed, 0.0).astype(out_ref.dtype)

    gather_own(0)
    slot_tables(place_ref, count_ref[0], table_v, row_blocks, positions)
    merged[slots] = jnp.zeros((tile, tile), merged.dtype)
    hidden[...] = jnp.dot(
        feat_ref[...], proj_ref[:width, :], preferred_element_type=jnp.float32) + bias_ref[...]
    for b in range(seg // LANES):
        one = degree_ref[b:b + 1, :].astype(jnp.float32)
        degree_col[b * LANES:(b + 1) * LANES, :] = jnp.transpose(jnp.broadcast_to(one, (LANES, LANES)))
    table_copy = pltpu.make_async_copy(table_v, table, table_sem)
    table_copy.start()
    forward(0)
    gather_own(1)
    table_copy.wait()
    for i in range(CHUNKS):
        load(i).wait()
    running = jnp.zeros((tile, tile), merged.dtype)
    for part in range(slots // LANES):
        def merge(i, running, part=part):
            keep = table[slots // LANES + part, i].astype(jnp.float32)
            kept = jnp.broadcast_to(keep, (16, tile)).astype(running.dtype)
            kept = jnp.concatenate([kept] * (tile // 16), axis=0)
            running = stage[table[part, i]] + running * kept
            merged[part * LANES + i] = running
            return running
        running = lax.fori_loop(0, LANES, merge, running, unroll=UNROLL)

    share_near(0)
    gather_copy(0, OWN_SIB).wait_recv()
    add_pair(0, (0, 1), True)
    gather_copy(0, SIB_X).wait_recv()
    add_pair(0, (2, 3), False)
    share_far(0)
    gather_copy(0, SIB_Y).wait_recv()
    add_pair(0, (4, 5), False)
    gather_copy(0, SIB_D).wait_recv()
    last_pair(0, 0)
    forward(1)
    last_pair(0, 1)
    last_pair(0, 2)
    share_near(1)
    own_segment(0)
    gather_copy(1, OWN_SIB).wait_recv()
    add_pair(1, (0, 1), True)
    share_far(1)
    gather_copy(1, SIB_X).wait_recv()
    add_pair(1, (2, 3), False)
    gather_copy(1, SIB_Y).wait_recv()
    add_pair(1, (4, 5), False)
    relay_sum(0, 0)
    gather_copy(1, SIB_D).wait_recv()
    for i in range(3):
        last_pair(1, i)
    relay_sum(0, 1)
    own_segment(1)
    finish(0)
    relay_sum(1, 0)
    relay_sum(1, 1)
    finish(1)

    for h in range(halves):
        for j in range(10):
            gather_copy(h, j).wait_send()
        for q in range(PIECES):
            for i in range(2):
                relay_copy(h, i, q).wait_send()
            near_copy(h, q).wait_send()


def local_fused(n_row, n_col, features, in_degree, tile_index, tile_count, adjacency_tiles, projection, out_bias):
    seg, width = features.shape
    slots, tile, _ = adjacency_tiles.shape
    halves = width // LANES
    positions = (seg * n_col // tile) * (seg * n_row // tile)
    lines = 2 * (slots // LANES) + positions // LANES
    vmem = pl.BlockSpec(memory_space=pltpu.VMEM)
    smem = pl.BlockSpec(memory_space=pltpu.SMEM)
    gather_sem = pltpu.SemaphoreType.DMA((halves, 10))
    return pl.pallas_call(
        fused_kernel,
        out_shape=jax.ShapeDtypeStruct((seg, projection.shape[1]), jnp.bfloat16),
        in_specs=[vmem, vmem, smem, pl.BlockSpec(memory_space=pl.ANY), vmem, vmem, vmem],
        out_specs=vmem,
        scratch_shapes=[
            pltpu.VMEM((slots, tile, tile), jnp.bfloat16),
            pltpu.VMEM((slots + 1, tile, tile), jnp.bfloat16),
            pltpu.VMEM((lines, LANES), jnp.int32),
            pltpu.SMEM((lines, LANES), jnp.int32),
            pltpu.VMEM((halves, n_row, seg, LANES), jnp.bfloat16),
            pltpu.VMEM((halves, n_col * seg, LANES), jnp.float32),
            pltpu.VMEM((seg, projection.shape[1]), jnp.float32),
            pltpu.VMEM((seg, LANES), jnp.float32),
            pltpu.VMEM((halves, 3, seg, LANES), jnp.bfloat16),
            pltpu.VMEM((halves, 2, seg, LANES), jnp.bfloat16),
            pltpu.VMEM((halves, 2, seg, LANES), jnp.bfloat16),
            pltpu.SemaphoreType.DMA((CHUNKS,)),
            pltpu.SemaphoreType.DMA,
            gather_sem, gather_sem,
            pltpu.SemaphoreType.DMA((halves, 3, PIECES)),
            pltpu.SemaphoreType.DMA((halves, 2, PIECES)),
            pltpu.SemaphoreType.DMA((halves, 2, PIECES)),
        ],
        compiler_params=pltpu.CompilerParams(
            collective_id=0, has_side_effects=True, vmem_limit_bytes=56 * 1024 * 1024),
    )(features, tile_index.T, tile_count, adjacency_tiles,
      in_degree.reshape(seg // LANES, LANES), projection, out_bias[None, :])


def solution(mesh):
    n_row, n_col = mesh.shape["row"], mesh.shape["col"]

    def local(features, in_degree, tile_index, tile_count, adjacency_tiles, projection, out_bias):
        seg, width = features.shape
        slots, tile, _ = adjacency_tiles.shape
        positions = (seg * n_col // LANES) * (seg * n_row // LANES)
        fits = (
            n_row == 8 and n_col == 4 and tile == LANES and slots <= 256 and slots % LANES == 0
            and 4 * slots * tile * tile <= MERGE_LIMIT
            and seg % (2 * LANES) == 0 and width == 2 * LANES and positions % LANES == 0
            and LANES % (positions // n_row) == 0)
        args = (features, in_degree, tile_index, tile_count, adjacency_tiles, projection, out_bias)
        return local_fused(n_row, n_col, *args) if fits else local_sparse(*args)

    return jax.shard_map(
        local,
        mesh=mesh,
        in_specs=(
            P(("row", "col"), None),
            P(("row", "col")),
            P(("row", "col"), None),
            P(("row", "col")),
            P(("row", "col"), None, None),
            P(),
            P(),
        ),
        out_specs=P(("row", "col"), None),
        check_vma=False,
    )
```

```python
import functools

import jax
import jax.numpy as jnp
from jax import lax
from jax.experimental import pallas as pl
from jax.experimental.pallas import tpu as pltpu
from jax.sharding import PartitionSpec as P

BLK = 32
LANES = 128
CHUNKS = 16
PIECES = 2
NEAR = 4
UNROLL = 8
MERGE_LIMIT = 20 * 1024 * 1024
MESH = pl.DeviceIdType.MESH


def block_terms(running, col_blocks, index_block, tile_block, live_block):
    picked = col_blocks[index_block[:, 1]]
    kept = jnp.where(live_block[:, None, None], tile_block, jnp.zeros_like(tile_block))
    product = jnp.einsum("kij,kjf->kif", kept, picked, preferred_element_type=jnp.float32)
    flattened = product.reshape(product.shape[0], -1)
    return running.at[index_block[:, 0]].add(flattened)


def local_sparse(features, in_degree, tile_index, tile_count, adjacency_tiles, projection, out_bias):
    feat_width = features.shape[1]
    tile_size = adjacency_tiles.shape[1]
    slot_total = adjacency_tiles.shape[0]
    gathered = lax.all_gather(features, "row", axis=0, tiled=True)
    col_blocks = gathered.reshape(gathered.shape[0] // tile_size, tile_size, feat_width)
    row_blocks = features.shape[0] * lax.axis_size("col") // tile_size
    live_count = tile_count[0]
    zeroed = jnp.zeros((row_blocks, tile_size * feat_width), jnp.float32)

    def one_step(running, offset):
        index_block = lax.dynamic_slice_in_dim(tile_index, offset, BLK, 0)
        tile_block = lax.dynamic_slice_in_dim(adjacency_tiles, offset, BLK, 0)
        live_block = offset + jnp.arange(BLK, dtype=jnp.int32) < live_count
        return (block_terms(running, col_blocks, index_block, tile_block, live_block), None)

    summed, _ = lax.scan(one_step, zeroed, jnp.arange(0, slot_total, BLK, dtype=jnp.int32))
    partial_value = summed.reshape(row_blocks * tile_size, feat_width)
    own_sums = lax.psum_scatter(partial_value, "col", scatter_dimension=0, tiled=True)
    neighbour_mean = (own_sums / in_degree[:, None].astype(jnp.float32)).astype(jnp.bfloat16)
    joined = jnp.concatenate([features, neighbour_mean], axis=1)
    mixed = jnp.dot(joined, projection, preferred_element_type=jnp.float32) + out_bias[None, :]
    return jnp.maximum(mixed, 0.0).astype(jnp.bfloat16)


def slot_tables(place_ref, count, table_ref, row_blocks, positions):
    slots = place_ref.shape[1]
    chunks = slots // LANES
    slot_row = lax.broadcasted_iota(jnp.int32, (1, slots), 1)
    spot_row = place_ref[1:2, :] * row_blocks + place_ref[0:1, :]
    spot_row = jnp.where(slot_row < count, spot_row, positions)

    def lane(v, i):
        return v[:, i * LANES:(i + 1) * LANES]

    spot = jnp.concatenate(
        [jnp.transpose(jnp.broadcast_to(lane(spot_row, i), (LANES, LANES))) for i in range(chunks)], axis=0)
    slot = lax.broadcasted_iota(jnp.int32, (slots, LANES), 0)
    before = jnp.zeros((slots, LANES), jnp.float32)
    repeat = jnp.zeros((slots, LANES), jnp.float32)
    for i in range(chunks):
        equal = lane(spot_row, i) == spot
        earlier = lane(slot_row, i) < slot
        first = (lane(spot_row, i) < spot) | (equal & earlier)
        before = before + jnp.where(first, 1.0, 0.0)
        repeat = jnp.maximum(repeat, jnp.where(equal & earlier, 1.0, 0.0))
    rank = jnp.sum(before, axis=1, keepdims=True).astype(jnp.int32)
    keep = jnp.max(repeat, axis=1, keepdims=True)
    for i in range(chunks):
        hit = rank == lax.broadcasted_iota(jnp.int32, (slots, LANES), 1) + i * LANES
        order = jnp.sum(jnp.where(hit, slot, 0), axis=0, keepdims=True)
        again = jnp.sum(jnp.where(hit, keep, 0.0), axis=0, keepdims=True)
        table_ref[i:i + 1, :] = order
        table_ref[chunks + i:chunks + i + 1, :] = again.astype(jnp.int32)
    for i in range(positions // LANES):
        here = lax.broadcasted_iota(jnp.int32, (slots, LANES), 1) + i * LANES
        upto = jnp.sum(jnp.where(spot <= here, 1, 0), axis=0, keepdims=True)
        count_here = jnp.sum(jnp.where(spot == here, 1, 0), axis=0, keepdims=True)
        table_ref[2 * chunks + i:2 * chunks + i + 1, :] = jnp.where(count_here > 0, upto - 1, slots)


def fused_kernel(feat_hbm, place_hbm, count_ref, tiles_ref, degree_hbm, proj_hbm, bias_hbm, out_ref,
                 feat_ref, place_ref, degree_ref, proj_ref, bias_ref,
                 stage, merged, table_v, table, gathered, acc, own, hidden, degree_col,
                 send, send_near, relayed, far, near_in,
                 in_sem, tile_sem, table_sem, ag_send, ag_recv,
                 send_sem, relay_sem, far_sem, near_send, near_recv):
    seg, width = feat_ref.shape
    slots, tile, _ = stage.shape
    halves = width // LANES
    blocks = seg // tile
    n_row, n_col = gathered.shape[1], 4
    row_blocks = n_col * blocks
    positions = blocks * n_row * row_blocks
    half_rows = seg // 2
    per = slots // CHUNKS
    r = lax.axis_index("row")
    c = lax.axis_index("col")
    near = c ^ 1
    upper = c < 2
    outer = (c == 0) | (c == 3)
    dests = (jnp.where(upper, 3, 0), jnp.where(upper, 2, 1), near, c)

    inputs = [(place_hbm, place_ref), (feat_hbm, feat_ref),
              (degree_hbm, degree_ref), (proj_hbm, proj_ref), (bias_hbm, bias_ref)]

    def fetch(i):
        return pltpu.make_async_copy(*inputs[i], in_sem.at[i])

    def load(i):
        part = pl.ds(i * per, per)
        return pltpu.make_async_copy(tiles_ref.at[part], stage.at[part], tile_sem.at[i])

    for i in range(2):
        fetch(i).start()

    barrier = pltpu.get_barrier_semaphore()

    def greet(row, col):
        pl.semaphore_signal(barrier, inc=1, device_id=(row, col), device_id_type=MESH)

    for m in (1, 2, 4):
        greet(r ^ m, c)
    greet(r, near)
    greet(r, c ^ 2)

    @pl.when(jnp.logical_not(outer))
    def _():
        greet(r, c ^ 3)

    for i in range(CHUNKS):
        load(i).start()
    for i in range(2, len(inputs)):
        fetch(i).start()

    OWN_SIB, OWN_XA, OWN_XB, OWN_YB, OWN_YA, FWD_Y, FWD_X, SIB_X, SIB_Y, SIB_D = range(10)
    first_rows, last_rows = pl.ds(0, half_rows), pl.ds(half_rows, half_rows)
    whole = pl.ds(0, seg)
    gather_plan = {
        OWN_SIB: (0, whole, 1), OWN_XA: (0, first_rows, 2), OWN_XB: (0, last_rows, 2),
        OWN_YB: (0, last_rows, 4), OWN_YA: (0, first_rows, 4),
        FWD_Y: (2, first_rows, 4), FWD_X: (4, last_rows, 2),
        SIB_X: (2, whole, 1), SIB_Y: (4, whole, 1), SIB_D: (6, whole, 1),
    }

    def lanes(h):
        return pl.ds(h * LANES, LANES)

    def gather_copy(h, j):
        flip, rows, step = gather_plan[j]
        owner = r ^ flip
        src = feat_ref.at[rows, lanes(h)] if flip == 0 else gathered.at[h, owner, rows, :]
        return pltpu.make_async_remote_copy(
            src_ref=src, dst_ref=gathered.at[h, owner, rows, :],
            send_sem=ag_send.at[h, j], recv_sem=ag_recv.at[h, j],
            device_id=(r ^ step, c), device_id_type=MESH)

    def gather_own(h):
        for j in (OWN_XA, OWN_YB, OWN_SIB, OWN_XB, OWN_YA):
            gather_copy(h, j).start()

    def forward(h):
        gather_copy(h, OWN_XA).wait_recv()
        gather_copy(h, FWD_Y).start()
        gather_copy(h, OWN_YB).wait_recv()
        gather_copy(h, FWD_X).start()

    def share_near(h):
        gather_copy(h, OWN_XB).wait_recv()
        gather_copy(h, SIB_X).start()
        gather_copy(h, OWN_YA).wait_recv()
        gather_copy(h, SIB_Y).start()

    def share_far(h):
        gather_copy(h, FWD_Y).wait_recv()
        gather_copy(h, FWD_X).wait_recv()
        gather_copy(h, SIB_D).start()

    def wait_for(h, j):
        gather_copy(h, j).wait_recv()

    def block_of(h, flip):
        if h is None:
            return jnp.concatenate([block_of(i, flip) for i in range(halves)], axis=1)
        return feat_ref[:, lanes(h)] if flip == 0 else gathered[h, r ^ flip]

    def product(h, flips, dest):
        columns = []
        for flip in flips:
            base = (r ^ flip) * (blocks * row_blocks)
            line = 2 * (slots // LANES) + base // LANES
            spot = base % LANES + dest * blocks
            columns += [(line, spot + k * row_blocks) for k in range(blocks)]
        left = jnp.concatenate(
            [jnp.concatenate([merged[table[line, spot + b]] for line, spot in columns], axis=1)
             for b in range(blocks)], axis=0)
        right = jnp.concatenate([block_of(h, flip) for flip in flips], axis=0)
        return jnp.dot(left, right, preferred_element_type=jnp.float32)

    def add_pair(h, flips, count, first):
        @pl.loop(0, count)
        def _(i):
            dest = jnp.where(i == 0, dests[0], dests[1])
            if first:
                acc[h, i] = product(h, flips, dest)
            else:
                acc[h, i] += product(h, flips, dest)

    def piece(q, pieces):
        return pl.ds(q * (seg // pieces), seg // pieces)

    def relay_copy(h, i, q):
        rows = piece(q, PIECES)
        return pltpu.make_async_remote_copy(
            src_ref=send.at[h, i, rows, :], dst_ref=relayed.at[h, i, rows, :],
            send_sem=send_sem.at[h, i, q], recv_sem=relay_sem.at[h, i, q],
            device_id=(r, near), device_id_type=MESH)

    def far_copy(h, i, q):
        rows = piece(q, PIECES)
        return pltpu.make_async_remote_copy(
            src_ref=send.at[h, i, rows, :], dst_ref=far.at[h, rows, :],
            send_sem=send_sem.at[h, i, q], recv_sem=far_sem.at[h, q],
            device_id=(r, dests[i]), device_id_type=MESH)

    def near_copy(q):
        rows = piece(q, NEAR)
        return pltpu.make_async_remote_copy(
            src_ref=send_near.at[rows, :], dst_ref=near_in.at[rows, :],
            send_sem=near_send.at[q], recv_sem=near_recv.at[q],
            device_id=(r, near), device_id_type=MESH)

    def last_pair(h, i):
        acc[h, i] += product(h, (6, 7), dests[i])

        @pl.when(outer)
        def _():
            for q in range(PIECES):
                rows = piece(q, PIECES)
                send[h, i, rows, :] = acc[h, i, rows, :].astype(send.dtype)
                relay_copy(h, i, q).start()

    def relay_sum(h, i, q):
        @pl.when(jnp.logical_not(outer))
        def _():
            rows = piece(q, PIECES)
            relay_copy(h, i, q).wait_recv()
            total = acc[h, i, rows, :] + relayed[h, i, rows, :].astype(jnp.float32)
            send[h, i, rows, :] = total.astype(send.dtype)
            far_copy(h, i, q).start()

    def near_segment():
        send_near[...] = product(None, range(n_row), near).astype(send_near.dtype)
        for q in range(NEAR):
            near_copy(q).start()

    def own_segment():
        own[...] = product(None, range(n_row), c)

    def finish():
        for q in range(NEAR):
            rows = piece(q, NEAR)
            if q % (NEAR // PIECES) == 0:
                for h in range(halves):
                    far_copy(h, 0, q // (NEAR // PIECES)).wait_recv()
            near_copy(q).wait_recv()
            divisor = degree_col[rows, :]
            mean = jnp.concatenate(
                [((own[rows, lanes(h)] + far[h, rows, :].astype(jnp.float32)
                   + near_in[rows, lanes(h)].astype(jnp.float32)) / divisor).astype(jnp.bfloat16)
                 for h in range(halves)], axis=1)
            mixed = hidden[rows, :] + jnp.dot(
                mean, proj_ref[width:, :], preferred_element_type=jnp.float32)
            out_ref[rows, :] = jnp.maximum(mixed, 0.0).astype(out_ref.dtype)

    def tables():
        fetch(0).wait()
        slot_tables(place_ref, count_ref[0], table_v, row_blocks, positions)

    table_copy = pltpu.make_async_copy(table_v, table, table_sem)

    def prepare():
        merged[slots] = jnp.zeros((tile, tile), merged.dtype)
        for i in range(2, len(inputs)):
            fetch(i).wait()
        hidden[...] = jnp.dot(
            feat_ref[...], proj_ref[:width, :], preferred_element_type=jnp.float32) + bias_ref[...]
        for b in range(seg // LANES):
            one = degree_ref[b:b + 1, :].astype(jnp.float32)
            degree_col[b * LANES:(b + 1) * LANES, :] = jnp.transpose(jnp.broadcast_to(one, (LANES, LANES)))

    def merge_slots(part, running):
        def merge(i, running):
            keep = table[slots // LANES + part, i].astype(jnp.float32)
            kept = jnp.broadcast_to(keep, (16, tile)).astype(running.dtype)
            kept = jnp.concatenate([kept] * (tile // 16), axis=0)
            running = stage[table[part, i]] + running * kept
            merged[part * LANES + i] = running
            return running
        return lax.fori_loop(0, LANES, merge, running, unroll=UNROLL)

    def wait_loads():
        table_copy.wait()
        for i in range(CHUNKS):
            load(i).wait()

    def step(name, run, *args):
        with jax.named_scope(name):
            return run(*args)

    step("tables", tables)
    step("w_feat", fetch(1).wait)
    step("barrier", pl.semaphore_wait, barrier, jnp.where(outer, 5, 6))
    step("own0", gather_own, 0)
    table_copy.start()
    step("prepare", prepare)
    step("loads", wait_loads)
    running = step("merge0", merge_slots, 0, jnp.zeros((tile, tile), merged.dtype))
    step("forward0", forward, 0)
    step("own1", gather_own, 1)
    for part in range(1, slots // LANES):
        running = step("merge1", merge_slots, part, running)
    step("share_near0", share_near, 0)
    step("w_sib0", wait_for, 0, OWN_SIB)
    step("pair0a", add_pair, 0, (0, 1), 2, True)
    step("w_x0", wait_for, 0, SIB_X)
    step("pair0x", add_pair, 0, (2, 3), 2, False)
    step("share_far0", share_far, 0)
    step("w_y0", wait_for, 0, SIB_Y)
    step("pair0y", add_pair, 0, (4, 5), 2, False)
    step("w_d0", wait_for, 0, SIB_D)
    step("last00", last_pair, 0, 0)
    step("forward1", forward, 1)
    step("last01", last_pair, 0, 1)
    step("w_sib1", wait_for, 1, OWN_SIB)
    step("pair1a", add_pair, 1, (0, 1), 2, True)
    step("share_near1", share_near, 1)
    step("relay000", relay_sum, 0, 0, 0)
    step("w_x1", wait_for, 1, SIB_X)
    step("pair1x", add_pair, 1, (2, 3), 2, False)
    step("share_far1", share_far, 1)
    step("w_y1", wait_for, 1, SIB_Y)
    step("pair1y", add_pair, 1, (4, 5), 2, False)
    step("relay001", relay_sum, 0, 0, 1)
    step("w_d1", wait_for, 1, SIB_D)
    step("last10", last_pair, 1, 0)
    step("last11", last_pair, 1, 1)
    step("relay010", relay_sum, 0, 1, 0)
    step("near_seg", near_segment)
    step("relay011", relay_sum, 0, 1, 1)
    step("relay100", relay_sum, 1, 0, 0)
    step("own_seg", own_segment)
    step("relay101", relay_sum, 1, 0, 1)
    step("relay110", relay_sum, 1, 1, 0)
    step("relay111", relay_sum, 1, 1, 1)
    step("finish", finish)

    for h in range(halves):
        for j in range(10):
            gather_copy(h, j).wait_send()
        for i in range(2):
            for q in range(PIECES):
                relay_copy(h, i, q).wait_send()
    for q in range(NEAR):
        near_copy(q).wait_send()


def local_fused(n_row, n_col, features, in_degree, tile_index, tile_count, adjacency_tiles, projection, out_bias):
    seg, width = features.shape
    slots, tile, _ = adjacency_tiles.shape
    halves = width // LANES
    positions = (seg * n_col // tile) * (seg * n_row // tile)
    lines = 2 * (slots // LANES) + positions // LANES
    hbm = pl.BlockSpec(memory_space=pltpu.HBM)
    gather_sem = pltpu.SemaphoreType.DMA((halves, 10))
    relay_sem = pltpu.SemaphoreType.DMA((halves, 2, PIECES))
    near_sem = pltpu.SemaphoreType.DMA((NEAR,))
    args = [features, tile_index.T, tile_count, adjacency_tiles,
            in_degree.reshape(seg // LANES, LANES), projection, out_bias[None, :]]
    specs = [hbm] * len(args)
    specs[2] = pl.BlockSpec(memory_space=pltpu.SMEM)
    args = [a if i == 2 else pltpu.with_memory_space_constraint(a, pltpu.HBM) for i, a in enumerate(args)]
    return pl.pallas_call(
        fused_kernel,
        out_shape=jax.ShapeDtypeStruct((seg, projection.shape[1]), jnp.bfloat16),
        in_specs=specs,
        out_specs=pl.BlockSpec(memory_space=pltpu.VMEM),
        scratch_shapes=[
            pltpu.VMEM(features.shape, features.dtype),
            pltpu.VMEM((2, slots), jnp.int32),
            pltpu.VMEM((seg // LANES, LANES), jnp.int32),
            pltpu.VMEM(projection.shape, projection.dtype),
            pltpu.VMEM((1, projection.shape[1]), jnp.float32),
            pltpu.VMEM((slots, tile, tile), jnp.bfloat16),
            pltpu.VMEM((slots + 1, tile, tile), jnp.bfloat16),
            pltpu.VMEM((lines, LANES), jnp.int32),
            pltpu.SMEM((lines, LANES), jnp.int32),
            pltpu.VMEM((halves, n_row, seg, LANES), jnp.bfloat16),
            pltpu.VMEM((halves, 2, seg, LANES), jnp.float32),
            pltpu.VMEM((seg, width), jnp.float32),
            pltpu.VMEM((seg, projection.shape[1]), jnp.float32),
            pltpu.VMEM((seg, LANES), jnp.float32),
            pltpu.VMEM((halves, 2, seg, LANES), jnp.bfloat16),
            pltpu.VMEM((seg, width), jnp.bfloat16),
            pltpu.VMEM((halves, 2, seg, LANES), jnp.bfloat16),
            pltpu.VMEM((halves, seg, LANES), jnp.bfloat16),
            pltpu.VMEM((seg, width), jnp.bfloat16),
            pltpu.SemaphoreType.DMA((len(args) - 2,)),
            pltpu.SemaphoreType.DMA((CHUNKS,)),
            pltpu.SemaphoreType.DMA,
            gather_sem, gather_sem,
            relay_sem, relay_sem, pltpu.SemaphoreType.DMA((halves, PIECES)),
            near_sem, near_sem,
        ],
        compiler_params=pltpu.CompilerParams(
            collective_id=0, has_side_effects=True, vmem_limit_bytes=48 * 1024 * 1024),
    )(*args)


def solution(mesh):
    n_row, n_col = mesh.shape["row"], mesh.shape["col"]

    def local(features, in_degree, tile_index, tile_count, adjacency_tiles, projection, out_bias):
        seg, width = features.shape
        slots, tile, _ = adjacency_tiles.shape
        positions = (seg * n_col // LANES) * (seg * n_row // LANES)
        fits = (
            n_row == 8 and n_col == 4 and tile == LANES and slots <= 256 and slots % LANES == 0
            and 4 * slots * tile * tile <= MERGE_LIMIT
            and seg % (2 * LANES) == 0 and width == 2 * LANES and positions % LANES == 0
            and LANES % (positions // n_row) == 0)
        args = (features, in_degree, tile_index, tile_count, adjacency_tiles, projection, out_bias)
        return local_fused(n_row, n_col, *args) if fits else local_sparse(*args)

    return jax.shard_map(
        local,
        mesh=mesh,
        in_specs=(
            P(("row", "col"), None),
            P(("row", "col")),
            P(("row", "col"), None),
            P(("row", "col")),
            P(("row", "col"), None, None),
            P(),
            P(),
        ),
        out_specs=P(("row", "col"), None),
        check_vma=False,
    )
```

```python
import functools

import jax
import jax.numpy as jnp
from jax import lax
from jax.experimental import pallas as pl
from jax.experimental.pallas import tpu as pltpu
from jax.sharding import PartitionSpec as P

BLK = 32
LANES = 128
CHUNKS = 16
PIECES = (2, 4)
NEAR = (1, 4)
ARRIVALS = 8
X, Y = 3, 5
UNROLL = 8
MERGE_LIMIT = 20 * 1024 * 1024
MESH = pl.DeviceIdType.MESH


def block_terms(running, col_blocks, index_block, tile_block, live_block):
    picked = col_blocks[index_block[:, 1]]
    kept = jnp.where(live_block[:, None, None], tile_block, jnp.zeros_like(tile_block))
    product = jnp.einsum("kij,kjf->kif", kept, picked, preferred_element_type=jnp.float32)
    flattened = product.reshape(product.shape[0], -1)
    return running.at[index_block[:, 0]].add(flattened)


def local_sparse(features, in_degree, tile_index, tile_count, adjacency_tiles, projection, out_bias):
    feat_width = features.shape[1]
    tile_size = adjacency_tiles.shape[1]
    slot_total = adjacency_tiles.shape[0]
    gathered = lax.all_gather(features, "row", axis=0, tiled=True)
    col_blocks = gathered.reshape(gathered.shape[0] // tile_size, tile_size, feat_width)
    row_blocks = features.shape[0] * lax.axis_size("col") // tile_size
    live_count = tile_count[0]
    zeroed = jnp.zeros((row_blocks, tile_size * feat_width), jnp.float32)

    def one_step(running, offset):
        index_block = lax.dynamic_slice_in_dim(tile_index, offset, BLK, 0)
        tile_block = lax.dynamic_slice_in_dim(adjacency_tiles, offset, BLK, 0)
        live_block = offset + jnp.arange(BLK, dtype=jnp.int32) < live_count
        return (block_terms(running, col_blocks, index_block, tile_block, live_block), None)

    summed, _ = lax.scan(one_step, zeroed, jnp.arange(0, slot_total, BLK, dtype=jnp.int32))
    partial_value = summed.reshape(row_blocks * tile_size, feat_width)
    own_sums = lax.psum_scatter(partial_value, "col", scatter_dimension=0, tiled=True)
    neighbour_mean = (own_sums / in_degree[:, None].astype(jnp.float32)).astype(jnp.bfloat16)
    joined = jnp.concatenate([features, neighbour_mean], axis=1)
    mixed = jnp.dot(joined, projection, preferred_element_type=jnp.float32) + out_bias[None, :]
    return jnp.maximum(mixed, 0.0).astype(jnp.bfloat16)


def slot_tables(place_ref, count, table_ref, row_blocks, positions):
    slots = place_ref.shape[1]
    chunks = slots // LANES
    slot_row = lax.broadcasted_iota(jnp.int32, (1, slots), 1)
    spot_row = place_ref[1:2, :] * row_blocks + place_ref[0:1, :]
    spot_row = jnp.where(slot_row < count, spot_row, positions)

    def lane(v, i):
        return v[:, i * LANES:(i + 1) * LANES]

    spot = jnp.concatenate(
        [jnp.transpose(jnp.broadcast_to(lane(spot_row, i), (LANES, LANES))) for i in range(chunks)], axis=0)
    slot = lax.broadcasted_iota(jnp.int32, (slots, LANES), 0)
    before = jnp.zeros((slots, LANES), jnp.float32)
    repeat = jnp.zeros((slots, LANES), jnp.float32)
    for i in range(chunks):
        equal = lane(spot_row, i) == spot
        earlier = lane(slot_row, i) < slot
        first = (lane(spot_row, i) < spot) | (equal & earlier)
        before = before + jnp.where(first, 1.0, 0.0)
        repeat = jnp.maximum(repeat, jnp.where(equal & earlier, 1.0, 0.0))
    rank = jnp.sum(before, axis=1, keepdims=True).astype(jnp.int32)
    keep = jnp.max(repeat, axis=1, keepdims=True)
    for i in range(chunks):
        hit = rank == lax.broadcasted_iota(jnp.int32, (slots, LANES), 1) + i * LANES
        order = jnp.sum(jnp.where(hit, slot, 0), axis=0, keepdims=True)
        again = jnp.sum(jnp.where(hit, keep, 0.0), axis=0, keepdims=True)
        table_ref[i:i + 1, :] = order
        table_ref[chunks + i:chunks + i + 1, :] = again.astype(jnp.int32)
    for i in range(positions // LANES):
        here = lax.broadcasted_iota(jnp.int32, (slots, LANES), 1) + i * LANES
        upto = jnp.sum(jnp.where(spot <= here, 1, 0), axis=0, keepdims=True)
        count_here = jnp.sum(jnp.where(spot == here, 1, 0), axis=0, keepdims=True)
        table_ref[2 * chunks + i:2 * chunks + i + 1, :] = jnp.where(count_here > 0, upto - 1, slots)


def fused_kernel(feat_hbm, place_hbm, count_ref, tiles_ref, degree_hbm, proj_hbm, bias_hbm, out_ref,
                 feat_ref, place_ref, degree_ref, proj_ref, bias_ref,
                 stage, merged, table_v, table, gathered, acc, own, hidden, degree_col,
                 send, send_near, relayed, far, near_in,
                 in_sem, tile_sem, table_sem, sent, ag_recv, relay_sem, far_sem, near_sem):
    seg, width = feat_ref.shape
    slots, tile, _ = stage.shape
    halves = width // LANES
    blocks = seg // tile
    n_row, n_col = gathered.shape[1], 4
    row_blocks = n_col * blocks
    positions = blocks * n_row * row_blocks
    half_rows, quarter = seg // 2, seg // 4
    per = slots // CHUNKS
    r = lax.axis_index("row")
    c = lax.axis_index("col")
    one = c // n_col + 1
    near = c ^ 1
    upper = c < 2
    outer = (c == 0) | (c == 3)
    dests = (jnp.where(upper, 3, 0), jnp.where(upper, 2, 1), near, c)

    inputs = [(feat_hbm, feat_ref), (place_hbm, place_ref),
              (degree_hbm, degree_ref), (proj_hbm, proj_ref), (bias_hbm, bias_ref)]

    def fetch(i):
        return pltpu.make_async_copy(*inputs[i], in_sem.at[i])

    for i in range(2):
        fetch(i).start()

    barrier = pltpu.get_barrier_semaphore()

    def greet(row, col):
        pl.semaphore_signal(barrier, inc=1, device_id=(row, col), device_id_type=MESH)

    for m in (1, X, Y):
        greet(r ^ m, c)
    greet(r, near)
    greet(r, c ^ 2)

    @pl.when(jnp.logical_not(outer))
    def _():
        greet(r, c ^ 3)

    for i in range(CHUNKS):
        part = pl.ds(i * per, per)
        pltpu.make_async_copy(tiles_ref.at[part], stage.at[part], tile_sem).start()
    for i in range(2, len(inputs)):
        fetch(i).start()

    rows_of = [pl.ds(i * quarter, quarter) for i in range(4)]
    first_rows, last_rows = pl.ds(0, half_rows), pl.ds(half_rows, half_rows)
    whole = pl.ds(0, seg)
    FROM_SIB, FROM_1, FROM_2, FROM_3, FROM_FAR, SIB_X, SIB_Y, SIB_D = range(ARRIVALS)
    arriving_rows = (seg, half_rows, half_rows, seg, seg, seg, seg, seg)

    def lanes(h):
        return pl.ds(h * LANES, LANES)

    def gather_start(h, flip, rows, step, arrival):
        owner = r ^ flip
        src = feat_ref.at[rows, lanes(h)] if flip == 0 else gathered.at[h, owner, rows, :]
        pltpu.make_async_remote_copy(
            src_ref=src, dst_ref=gathered.at[h, owner, rows, :],
            send_sem=sent, recv_sem=ag_recv.at[h, arrival],
            device_id=(r ^ step, c), device_id_type=MESH).start()

    def wait_for(h, arrival):
        rows = pl.ds(0, arriving_rows[arrival])
        pltpu.make_async_remote_copy(
            src_ref=gathered.at[h, 0, rows, :], dst_ref=gathered.at[h, 0, rows, :],
            send_sem=sent, recv_sem=ag_recv.at[h, arrival],
            device_id=(r ^ 1, c), device_id_type=MESH).wait_recv()

    def gather_own(h):
        gather_start(h, 0, rows_of[0], X, FROM_1)
        gather_start(h, 0, rows_of[2], Y, FROM_1)
        gather_start(h, 0, whole, 1, FROM_SIB)
        gather_start(h, 0, rows_of[1], X, FROM_2)
        gather_start(h, 0, rows_of[3], Y, FROM_2)
        gather_start(h, 0, last_rows, X, FROM_3)
        gather_start(h, 0, first_rows, Y, FROM_3)

    def forward(h, part):
        wait_for(h, (FROM_1, FROM_2)[part])
        gather_start(h, X, rows_of[part], Y, FROM_FAR)
        gather_start(h, Y, rows_of[2 + part], X, FROM_FAR)

    def share_near(h):
        wait_for(h, FROM_3)
        gather_start(h, X, whole, 1, SIB_X)
        gather_start(h, Y, whole, 1, SIB_Y)

    def share_far(h):
        wait_for(h, FROM_FAR)
        gather_start(h, 6, whole, 1, SIB_D)

    def block_of(h, flip):
        if h is None:
            return jnp.concatenate([block_of(i, flip) for i in range(halves)], axis=1)
        return feat_ref[:, lanes(h)] if flip == 0 else gathered[h, r ^ flip]

    def product(h, flips, dest, group=None):
        columns = []
        for flip in flips:
            base = (r ^ flip) * (blocks * row_blocks)
            line = 2 * (slots // LANES) + base // LANES
            spot = base % LANES + dest * blocks
            columns += [(line, spot + k * row_blocks) for k in range(blocks)]
        picks = range(blocks) if group is None else [group * (blocks // 2) + k for k in range(blocks // 2)]
        left = jnp.concatenate(
            [jnp.concatenate([merged[table[line, spot + b]] for line, spot in columns], axis=1)
             for b in picks], axis=0)
        right = jnp.concatenate([block_of(h, flip) for flip in flips], axis=0)
        return jnp.dot(left, right, preferred_element_type=jnp.float32)

    def half_of(g):
        return pl.ds(pl.multiple_of(g * half_rows, half_rows), half_rows)

    def add_pair(h, flips, low, count):
        @pl.loop(low, low + count)
        def _(i):
            dest = jnp.where(i == 0, dests[0], dests[1])
            if flips[0] == 0:
                acc[h, i] = product(h, flips, dest)
            else:
                acc[h, i] += product(h, flips, dest)

    def piece(q, pieces):
        size = seg // pieces
        return pl.ds(pl.multiple_of(q * size, size), size)

    def sum_copy(src, dst, recv, row, col):
        return pltpu.make_async_remote_copy(
            src_ref=src, dst_ref=dst, send_sem=sent, recv_sem=recv,
            device_id=(row, col), device_id_type=MESH)

    def relay_copy(h, i, q):
        rows = piece(q, PIECES[h])
        return sum_copy(send.at[h, i, rows, :], relayed.at[h, i, rows, :],
                        relay_sem.at[2 * sum(PIECES[:h]) + i * PIECES[h] + q], r, near)

    def far_copy(h, i, q):
        rows = piece(q, PIECES[h])
        return sum_copy(send.at[h, i, rows, :], far.at[h, rows, :],
                        far_sem.at[0 if h == 0 else q + 1], r, dests[i])

    def near_copy(h, q):
        rows = piece(q, NEAR[h])
        return sum_copy(send_near.at[h, rows, :], near_in.at[h, rows, :],
                        near_sem.at[sum(NEAR[:h]) + q], r, near)

    def last_pair(h, i):
        each = PIECES[h] // 2

        @pl.loop(0, 2)
        def _(g):
            rows = half_of(g)
            total = acc[h, i, rows, :] + product(h, (6, 7), dests[i], g)
            acc[h, i, rows, :] = total

            @pl.when(outer)
            def _():
                send[h, i, rows, :] = total.astype(send.dtype)
                for k in range(each):
                    relay_copy(h, i, g * each + k).start()

    def relay_sum(h, i, q):
        @pl.when(jnp.logical_not(outer))
        def _():
            rows = piece(q, PIECES[h])
            relay_copy(h, i, q).wait_recv()
            total = acc[h, i, rows, :] + relayed[h, i, rows, :].astype(jnp.float32)
            send[h, i, rows, :] = total.astype(send.dtype)
            far_copy(h, i, q).start()

    def near_segment(h):
        @pl.loop(0, 2)
        def _(g):
            rows = half_of(g)
            send_near[h, rows, :] = product(h, range(n_row), near, g).astype(send_near.dtype)
        for q in range(NEAR[h]):
            near_copy(h, q).start()

    def own_segment():
        @pl.loop(0, 2)
        def _(g):
            own[half_of(g), :] = product(None, range(n_row), c, g)

    def finish():
        sum_copy(far.at[0], far.at[0], far_sem.at[0], r, near).wait_recv()
        near_copy(0, 0).wait_recv()
        pieces = NEAR[1]
        for q in range(pieces):
            rows = piece(q, pieces)
            far_copy(1, 0, q).wait_recv()
            near_copy(1, q).wait_recv()
            divisor = degree_col[rows, :]
            mean = jnp.concatenate(
                [((own[rows, lanes(h)] + far[h, rows, :].astype(jnp.float32)
                   + near_in[h, rows, :].astype(jnp.float32)) / divisor).astype(jnp.bfloat16)
                 for h in range(halves)], axis=1)
            mixed = hidden[rows, :] + jnp.dot(
                mean, proj_ref[width:, :], preferred_element_type=jnp.float32)
            out_ref[rows, :] = jnp.maximum(mixed, 0.0).astype(out_ref.dtype)

    def tables():
        fetch(1).wait()
        merged[slots] = jnp.zeros((tile, tile), merged.dtype)
        slot_tables(place_ref, count_ref[0], table_v, row_blocks, positions)

    table_copy = pltpu.make_async_copy(table_v, table, table_sem)

    def wait_loads():
        table_copy.wait()
        pltpu.make_async_copy(tiles_ref, stage, tile_sem).wait()

    def merge_slots(low, high, running):
        for part in range(slots // LANES):
            def merge(i, running, part=part):
                keep = table[slots // LANES + part, i].astype(jnp.float32)
                kept = jnp.broadcast_to(keep, (16, tile)).astype(running.dtype)
                kept = jnp.concatenate([kept] * (tile // 16), axis=0)
                running = stage[table[part, i]] + running * kept
                merged[part * LANES + i] = running
                return running
            begin, end = max(low - part * LANES, 0), min(high - part * LANES, LANES)
            if begin < end:
                running = lax.fori_loop(begin, end, merge, running, unroll=UNROLL)
        return running

    def prepare():
        for i in range(2, len(inputs)):
            fetch(i).wait()
        hidden[...] = jnp.dot(
            feat_ref[...], proj_ref[:width, :], preferred_element_type=jnp.float32) + bias_ref[...]
        for b in range(seg // LANES):
            one = degree_ref[b:b + 1, :].astype(jnp.float32)
            degree_col[b * LANES:(b + 1) * LANES, :] = jnp.transpose(jnp.broadcast_to(one, (LANES, LANES)))

    def drain():
        tiles_sent = halves * 10 * seg * LANES // (tile * tile)
        sum_copy(stage.at[pl.ds(0, tiles_sent)], stage.at[pl.ds(0, tiles_sent)],
                 near_sem.at[0], r, near).wait_send()

    def step(name, run, *args):
        with jax.named_scope(name):
            return run(*args)

    early = slots // 4
    step("w_feat", fetch(0).wait)
    step("barrier", pl.semaphore_wait, barrier, jnp.where(outer, 5, 6))
    step("own0", gather_own, 0)
    step("tables", tables)
    table_copy.start()
    step("loads", wait_loads)
    step("forward0a", forward, 0, 0)
    running = step("merge0", merge_slots, 0, early, jnp.zeros((tile, tile), merged.dtype))
    step("forward0b", forward, 0, 1)
    step("own1", gather_own, 1)
    step("merge1", merge_slots, early, slots, running)
    step("w_sib0", wait_for, 0, FROM_SIB)
    step("pair0a0", add_pair, 0, (0, 1), 0, one)
    step("share_near0", share_near, 0)
    step("pair0a1", add_pair, 0, (0, 1), 1, one)
    step("share_far0", share_far, 0)
    step("w_x0", wait_for, 0, SIB_X)
    step("pair0x0", add_pair, 0, (2, 3), 0, one)
    step("w_y0", wait_for, 0, SIB_Y)
    step("pair0y0", add_pair, 0, (4, 5), 0, one)
    step("w_d0", wait_for, 0, SIB_D)
    step("last00", last_pair, 0, 0)
    step("forward1a", forward, 1, 0)
    step("pair0x1", add_pair, 0, (2, 3), 1, one)
    step("forward1b", forward, 1, 1)
    step("pair0y1", add_pair, 0, (4, 5), 1, one)
    step("last01", last_pair, 0, 1)
    step("near_seg0", near_segment, 0)
    step("w_sib1", wait_for, 1, FROM_SIB)
    step("pair1a", add_pair, 1, (0, 1), 0, 2)
    step("share_near1", share_near, 1)
    step("w_x1", wait_for, 1, SIB_X)
    step("pair1x", add_pair, 1, (2, 3), 0, 2)
    step("share_far1", share_far, 1)
    step("w_y1", wait_for, 1, SIB_Y)
    step("pair1y", add_pair, 1, (4, 5), 0, 2)
    step("relay000", relay_sum, 0, 0, 0)
    step("w_d1", wait_for, 1, SIB_D)
    step("last10", last_pair, 1, 0)
    step("last11", last_pair, 1, 1)
    step("relay001", relay_sum, 0, 0, 1)
    step("relay010", relay_sum, 0, 1, 0)
    step("near_seg1", near_segment, 1)
    step("relay011", relay_sum, 0, 1, 1)
    step("own_seg", own_segment)
    step("prepare", prepare)
    for i in range(2):
        for q in range(PIECES[1]):
            step("relay1", relay_sum, 1, i, q)
    step("finish", finish)
    step("drain", drain)


def local_fused(n_row, n_col, features, in_degree, tile_index, tile_count, adjacency_tiles, projection, out_bias):
    seg, width = features.shape
    slots, tile, _ = adjacency_tiles.shape
    halves = width // LANES
    positions = (seg * n_col // tile) * (seg * n_row // tile)
    lines = 2 * (slots // LANES) + positions // LANES
    hbm = pl.BlockSpec(memory_space=pltpu.HBM)
    args = [features, tile_index.T, tile_count, adjacency_tiles,
            in_degree.reshape(seg // LANES, LANES), projection, out_bias[None, :]]
    specs = [hbm] * len(args)
    specs[2] = pl.BlockSpec(memory_space=pltpu.SMEM)
    args = [a if i == 2 else pltpu.with_memory_space_constraint(a, pltpu.HBM) for i, a in enumerate(args)]
    return pl.pallas_call(
        fused_kernel,
        out_shape=jax.ShapeDtypeStruct((seg, projection.shape[1]), jnp.bfloat16),
        in_specs=specs,
        out_specs=pl.BlockSpec(memory_space=pltpu.VMEM),
        scratch_shapes=[
            pltpu.VMEM(features.shape, features.dtype),
            pltpu.VMEM((2, slots), jnp.int32),
            pltpu.VMEM((seg // LANES, LANES), jnp.int32),
            pltpu.VMEM(projection.shape, projection.dtype),
            pltpu.VMEM((1, projection.shape[1]), jnp.float32),
            pltpu.VMEM((slots, tile, tile), jnp.bfloat16),
            pltpu.VMEM((slots + 1, tile, tile), jnp.bfloat16),
            pltpu.VMEM((lines, LANES), jnp.int32),
            pltpu.SMEM((lines, LANES), jnp.int32),
            pltpu.VMEM((halves, n_row, seg, LANES), jnp.bfloat16),
            pltpu.VMEM((halves, 2, seg, LANES), jnp.float32),
            pltpu.VMEM((seg, width), jnp.float32),
            pltpu.VMEM((seg, projection.shape[1]), jnp.float32),
            pltpu.VMEM((seg, LANES), jnp.float32),
            pltpu.VMEM((halves, 2, seg, LANES), jnp.bfloat16),
            pltpu.VMEM((halves, seg, LANES), jnp.bfloat16),
            pltpu.VMEM((halves, 2, seg, LANES), jnp.bfloat16),
            pltpu.VMEM((halves, seg, LANES), jnp.bfloat16),
            pltpu.VMEM((halves, seg, LANES), jnp.bfloat16),
            pltpu.SemaphoreType.DMA((len(args) - 2,)),
            pltpu.SemaphoreType.DMA,
            pltpu.SemaphoreType.DMA,
            pltpu.SemaphoreType.DMA,
            pltpu.SemaphoreType.DMA((halves, ARRIVALS)),
            pltpu.SemaphoreType.DMA((2 * sum(PIECES),)),
            pltpu.SemaphoreType.DMA((1 + PIECES[1],)),
            pltpu.SemaphoreType.DMA((sum(NEAR),)),
        ],
        compiler_params=pltpu.CompilerParams(
            collective_id=0, has_side_effects=True, vmem_limit_bytes=48 * 1024 * 1024),
    )(*args)


def solution(mesh):
    n_row, n_col = mesh.shape["row"], mesh.shape["col"]

    def local(features, in_degree, tile_index, tile_count, adjacency_tiles, projection, out_bias):
        seg, width = features.shape
        slots, tile, _ = adjacency_tiles.shape
        positions = (seg * n_col // LANES) * (seg * n_row // LANES)
        fits = (
            n_row == 8 and n_col == 4 and tile == LANES and slots <= 256 and slots % LANES == 0
            and 4 * slots * tile * tile <= MERGE_LIMIT
            and seg % (4 * LANES) == 0 and width == 2 * LANES and positions % LANES == 0
            and LANES % (positions // n_row) == 0)
        args = (features, in_degree, tile_index, tile_count, adjacency_tiles, projection, out_bias)
        return local_fused(n_row, n_col, *args) if fits else local_sparse(*args)

    return jax.shard_map(
        local,
        mesh=mesh,
        in_specs=(
            P(("row", "col"), None),
            P(("row", "col")),
            P(("row", "col"), None),
            P(("row", "col")),
            P(("row", "col"), None, None),
            P(),
            P(),
        ),
        out_specs=P(("row", "col"), None),
        check_vma=False,
    )
```

```python
import functools

import jax
import jax.numpy as jnp
from jax import lax
from jax.experimental import pallas as pl
from jax.experimental.pallas import tpu as pltpu
from jax.sharding import PartitionSpec as P

BLK = 32
LANES = 128
CHUNKS = 16
PIECES = (2, 4)
NEAR = (2, 4)
ARRIVALS = 6
X, Y = 3, 5
UNROLL = 8
MERGE_LIMIT = 20 * 1024 * 1024
MESH = pl.DeviceIdType.MESH


def block_terms(running, col_blocks, index_block, tile_block, live_block):
    picked = col_blocks[index_block[:, 1]]
    kept = jnp.where(live_block[:, None, None], tile_block, jnp.zeros_like(tile_block))
    product = jnp.einsum("kij,kjf->kif", kept, picked, preferred_element_type=jnp.float32)
    flattened = product.reshape(product.shape[0], -1)
    return running.at[index_block[:, 0]].add(flattened)


def local_sparse(features, in_degree, tile_index, tile_count, adjacency_tiles, projection, out_bias):
    feat_width = features.shape[1]
    tile_size = adjacency_tiles.shape[1]
    slot_total = adjacency_tiles.shape[0]
    gathered = lax.all_gather(features, "row", axis=0, tiled=True)
    col_blocks = gathered.reshape(gathered.shape[0] // tile_size, tile_size, feat_width)
    row_blocks = features.shape[0] * lax.axis_size("col") // tile_size
    live_count = tile_count[0]
    zeroed = jnp.zeros((row_blocks, tile_size * feat_width), jnp.float32)

    def one_step(running, offset):
        index_block = lax.dynamic_slice_in_dim(tile_index, offset, BLK, 0)
        tile_block = lax.dynamic_slice_in_dim(adjacency_tiles, offset, BLK, 0)
        live_block = offset + jnp.arange(BLK, dtype=jnp.int32) < live_count
        return (block_terms(running, col_blocks, index_block, tile_block, live_block), None)

    summed, _ = lax.scan(one_step, zeroed, jnp.arange(0, slot_total, BLK, dtype=jnp.int32))
    partial_value = summed.reshape(row_blocks * tile_size, feat_width)
    own_sums = lax.psum_scatter(partial_value, "col", scatter_dimension=0, tiled=True)
    neighbour_mean = (own_sums / in_degree[:, None].astype(jnp.float32)).astype(jnp.bfloat16)
    joined = jnp.concatenate([features, neighbour_mean], axis=1)
    mixed = jnp.dot(joined, projection, preferred_element_type=jnp.float32) + out_bias[None, :]
    return jnp.maximum(mixed, 0.0).astype(jnp.bfloat16)


def slot_tables(place_ref, count, table_ref, row_blocks, positions):
    slots = place_ref.shape[1]
    chunks = slots // LANES
    slot_row = lax.broadcasted_iota(jnp.int32, (1, slots), 1)
    spot_row = place_ref[1:2, :] * row_blocks + place_ref[0:1, :]
    spot_row = jnp.where(slot_row < count, spot_row, positions)

    def lane(v, i):
        return v[:, i * LANES:(i + 1) * LANES]

    spot = jnp.concatenate(
        [jnp.transpose(jnp.broadcast_to(lane(spot_row, i), (LANES, LANES))) for i in range(chunks)], axis=0)
    slot = lax.broadcasted_iota(jnp.int32, (slots, LANES), 0)
    before = jnp.zeros((slots, LANES), jnp.float32)
    repeat = jnp.zeros((slots, LANES), jnp.float32)
    for i in range(chunks):
        equal = lane(spot_row, i) == spot
        earlier = lane(slot_row, i) < slot
        first = (lane(spot_row, i) < spot) | (equal & earlier)
        before = before + jnp.where(first, 1.0, 0.0)
        repeat = jnp.maximum(repeat, jnp.where(equal & earlier, 1.0, 0.0))
    rank = jnp.sum(before, axis=1, keepdims=True).astype(jnp.int32)
    keep = jnp.max(repeat, axis=1, keepdims=True)
    for i in range(chunks):
        hit = rank == lax.broadcasted_iota(jnp.int32, (slots, LANES), 1) + i * LANES
        order = jnp.sum(jnp.where(hit, slot, 0), axis=0, keepdims=True)
        again = jnp.sum(jnp.where(hit, keep, 0.0), axis=0, keepdims=True)
        table_ref[i:i + 1, :] = order
        table_ref[chunks + i:chunks + i + 1, :] = again.astype(jnp.int32)
    for i in range(positions // LANES):
        here = lax.broadcasted_iota(jnp.int32, (slots, LANES), 1) + i * LANES
        upto = jnp.sum(jnp.where(spot <= here, 1, 0), axis=0, keepdims=True)
        count_here = jnp.sum(jnp.where(spot == here, 1, 0), axis=0, keepdims=True)
        table_ref[2 * chunks + i:2 * chunks + i + 1, :] = jnp.where(count_here > 0, upto - 1, slots)


def fused_kernel(feat_hbm, place_hbm, count_ref, tiles_ref, degree_hbm, proj_hbm, bias_hbm, out_ref,
                 feat_ref, place_ref, degree_ref, proj_ref, bias_ref,
                 stage, merged, table_v, table, gathered, acc, own, hidden, degree_col,
                 send, send_near, relayed, far, near_in,
                 in_sem, tile_sem, table_sem, sent, ag_recv, relay_sem, far_sem, near_sem):
    seg, width = feat_ref.shape
    slots, tile, _ = stage.shape
    halves = width // LANES
    blocks = seg // tile
    n_row, n_col = gathered.shape[1], 4
    row_blocks = n_col * blocks
    positions = blocks * n_row * row_blocks
    half_rows, quarter = seg // 2, seg // 4
    per = slots // CHUNKS
    r = lax.axis_index("row")
    c = lax.axis_index("col")
    one = c // n_col + 1
    near = c ^ 1
    upper = c < 2
    outer = (c == 0) | (c == 3)
    dests = (jnp.where(upper, 3, 0), jnp.where(upper, 2, 1), near, c)

    inputs = [(feat_hbm, feat_ref), (place_hbm, place_ref),
              (degree_hbm, degree_ref), (proj_hbm, proj_ref), (bias_hbm, bias_ref)]

    def fetch(i):
        return pltpu.make_async_copy(*inputs[i], in_sem.at[i])

    for i in range(2):
        fetch(i).start()

    barrier = pltpu.get_barrier_semaphore()

    def greet(row, col):
        pl.semaphore_signal(barrier, inc=1, device_id=(row, col), device_id_type=MESH)

    for m in (1, X, Y):
        greet(r ^ m, c)
    greet(r, near)
    greet(r, c ^ 2)

    @pl.when(jnp.logical_not(outer))
    def _():
        greet(r, c ^ 3)

    for i in range(2, len(inputs)):
        fetch(i).start()
    for i in range(CHUNKS):
        part = pl.ds(i * per, per)
        pltpu.make_async_copy(tiles_ref.at[part], stage.at[part], tile_sem).start()

    rows_of = [pl.ds(i * quarter, quarter) for i in range(4)]
    first_rows, last_rows = pl.ds(0, half_rows), pl.ds(half_rows, half_rows)
    whole = pl.ds(0, seg)
    FROM_1, FROM_2, FROM_3, FROM_FAR, SIB_XY, SIB_D = range(ARRIVALS)
    arriving_rows = (half_rows, half_rows, 2 * seg, seg, 2 * seg, seg)

    def lanes(h):
        return pl.ds(h * LANES, LANES)

    def gather_start(h, flip, rows, step, arrival):
        owner = r ^ flip
        src = feat_ref.at[rows, lanes(h)] if flip == 0 else gathered.at[h, owner, rows, :]
        pltpu.make_async_remote_copy(
            src_ref=src, dst_ref=gathered.at[h, owner, rows, :],
            send_sem=sent, recv_sem=ag_recv.at[h, arrival],
            device_id=(r ^ step, c), device_id_type=MESH).start()

    def wait_for(h, arrival):
        rows = arriving_rows[arrival]
        if rows <= seg:
            ref = gathered.at[h, 0, pl.ds(0, rows), :]
        else:
            ref = gathered.at[h, pl.ds(0, rows // seg)]
        pltpu.make_async_remote_copy(
            src_ref=ref, dst_ref=ref,
            send_sem=sent, recv_sem=ag_recv.at[h, arrival],
            device_id=(r ^ 1, c), device_id_type=MESH).wait_recv()

    def gather_own(h):
        gather_start(h, 0, rows_of[0], X, FROM_1)
        gather_start(h, 0, rows_of[2], Y, FROM_1)
        gather_start(h, 0, whole, 1, FROM_3)
        gather_start(h, 0, rows_of[1], X, FROM_2)
        gather_start(h, 0, rows_of[3], Y, FROM_2)
        gather_start(h, 0, last_rows, X, FROM_3)
        gather_start(h, 0, first_rows, Y, FROM_3)

    def forward(h, part):
        wait_for(h, (FROM_1, FROM_2)[part])
        gather_start(h, X, rows_of[part], Y, FROM_FAR)
        gather_start(h, Y, rows_of[2 + part], X, FROM_FAR)

    def share_near(h):
        wait_for(h, FROM_3)
        gather_start(h, X, whole, 1, SIB_XY)
        gather_start(h, Y, whole, 1, SIB_XY)

    def share_far(h):
        wait_for(h, FROM_FAR)
        gather_start(h, 6, whole, 1, SIB_D)

    def block_of(h, flip):
        if h is None:
            return jnp.concatenate([block_of(i, flip) for i in range(halves)], axis=1)
        return feat_ref[:, lanes(h)] if flip == 0 else gathered[h, r ^ flip]

    def product(h, flips, dest, group=None):
        columns = []
        for flip in flips:
            base = (r ^ flip) * (blocks * row_blocks)
            line = 2 * (slots // LANES) + base // LANES
            spot = base % LANES + dest * blocks
            columns += [(line, spot + k * row_blocks) for k in range(blocks)]
        picks = range(blocks) if group is None else [group * (blocks // 2) + k for k in range(blocks // 2)]
        left = jnp.concatenate(
            [jnp.concatenate([merged[table[line, spot + b]] for line, spot in columns], axis=1)
             for b in picks], axis=0)
        right = jnp.concatenate([block_of(h, flip) for flip in flips], axis=0)
        return jnp.dot(left, right, preferred_element_type=jnp.float32)

    def half_of(g):
        return pl.ds(pl.multiple_of(g * half_rows, half_rows), half_rows)

    def add_pair(h, flips, low, count):
        @pl.loop(low, low + count)
        def _(i):
            dest = jnp.where(i == 0, dests[0], dests[1])
            if flips[0] == 0:
                acc[h, i] = product(h, flips, dest)
            else:
                acc[h, i] += product(h, flips, dest)

    def piece(q, pieces):
        size = seg // pieces
        return pl.ds(pl.multiple_of(q * size, size), size)

    def sum_copy(src, dst, recv, row, col):
        return pltpu.make_async_remote_copy(
            src_ref=src, dst_ref=dst, send_sem=sent, recv_sem=recv,
            device_id=(row, col), device_id_type=MESH)

    def relay_copy(h, i, q):
        rows = piece(q, PIECES[h])
        return sum_copy(send.at[h, i, rows, :], relayed.at[h, i, rows, :],
                        relay_sem.at[2 * sum(PIECES[:h]) + i * PIECES[h] + q], r, near)

    def far_copy(h, i, q):
        rows = piece(q, PIECES[h])
        return sum_copy(send.at[h, i, rows, :], far.at[h, rows, :],
                        far_sem.at[0 if h == 0 else q + 1], r, dests[i])

    def near_copy(h, q):
        rows = piece(q, NEAR[h])
        return sum_copy(send_near.at[h, rows, :], near_in.at[h, rows, :],
                        near_sem.at[0 if h == 0 else q + 1], r, near)

    def last_pair(h, i):
        each = PIECES[h] // 2

        @pl.loop(0, 2)
        def _(g):
            rows = half_of(g)
            total = acc[h, i, rows, :] + product(h, (6, 7), dests[i], g)
            acc[h, i, rows, :] = total

            @pl.when(outer)
            def _():
                send[h, i, rows, :] = total.astype(send.dtype)
                for k in range(each):
                    relay_copy(h, i, g * each + k).start()

    def relay_sum(h, i, q):
        @pl.when(jnp.logical_not(outer))
        def _():
            rows = piece(q, PIECES[h])
            relay_copy(h, i, q).wait_recv()
            total = acc[h, i, rows, :] + relayed[h, i, rows, :].astype(jnp.float32)
            send[h, i, rows, :] = total.astype(send.dtype)
            far_copy(h, i, q).start()

    def near_product(h, trips):
        @pl.loop(0, trips)
        def _(g):
            rows = half_of(g)
            send_near[h, rows, :] = product(h, range(n_row), near, g).astype(send_near.dtype)

    def near_segment(mine):
        near_product(1, jnp.where(mine, 2, 0))

        @pl.when(mine)
        def _():
            for q in range(NEAR[1]):
                near_copy(1, q).start()

    def near_first():
        near_product(0, 2)
        near_copy(0, 0).start()

        @pl.when(jnp.logical_not(outer))
        def _():
            near_copy(0, 1).start()

    def near_rest():
        @pl.when(outer)
        def _():
            near_copy(0, 1).start()

    def own_segment():
        @pl.loop(0, 2)
        def _(g):
            own[half_of(g), :] = product(None, range(n_row), c, g)

    def finish():
        sum_copy(far.at[0], far.at[0], far_sem.at[0], r, near).wait_recv()
        sum_copy(near_in.at[0], near_in.at[0], near_sem.at[0], r, near).wait_recv()
        pieces = NEAR[1]
        for q in range(pieces):
            rows = piece(q, pieces)
            far_copy(1, 0, q).wait_recv()
            near_copy(1, q).wait_recv()
            divisor = degree_col[rows, :]
            mean = jnp.concatenate(
                [((own[rows, lanes(h)] + far[h, rows, :].astype(jnp.float32)
                   + near_in[h, rows, :].astype(jnp.float32)) / divisor).astype(jnp.bfloat16)
                 for h in range(halves)], axis=1)
            mixed = hidden[rows, :] + jnp.dot(
                mean, proj_ref[width:, :], preferred_element_type=jnp.float32)
            out_ref[rows, :] = jnp.maximum(mixed, 0.0).astype(out_ref.dtype)

    def tables():
        fetch(1).wait()
        merged[slots] = jnp.zeros((tile, tile), merged.dtype)
        slot_tables(place_ref, count_ref[0], table_v, row_blocks, positions)

    table_copy = pltpu.make_async_copy(table_v, table, table_sem)

    def wait_loads():
        table_copy.wait()
        pltpu.make_async_copy(tiles_ref, stage, tile_sem).wait()

    def merge_slots(low, high, running):
        for part in range(slots // LANES):
            def merge(i, running, part=part):
                keep = table[slots // LANES + part, i].astype(jnp.float32)
                kept = jnp.broadcast_to(keep, (16, tile)).astype(running.dtype)
                kept = jnp.concatenate([kept] * (tile // 16), axis=0)
                running = stage[table[part, i]] + running * kept
                merged[part * LANES + i] = running
                return running
            begin, end = max(low - part * LANES, 0), min(high - part * LANES, LANES)
            if begin < end:
                running = lax.fori_loop(begin, end, merge, running, unroll=UNROLL)
        return running

    def prepare():
        for i in range(2, len(inputs)):
            fetch(i).wait()
        hidden[...] = jnp.dot(
            feat_ref[...], proj_ref[:width, :], preferred_element_type=jnp.float32) + bias_ref[...]
        for b in range(seg // LANES):
            one = degree_ref[b:b + 1, :].astype(jnp.float32)
            degree_col[b * LANES:(b + 1) * LANES, :] = jnp.transpose(jnp.broadcast_to(one, (LANES, LANES)))

    def drain():
        tiles_sent = halves * 10 * seg * LANES // (tile * tile)
        sum_copy(stage.at[pl.ds(0, tiles_sent)], stage.at[pl.ds(0, tiles_sent)],
                 near_sem.at[0], r, near).wait_send()

    def step(name, run, *args):
        with jax.named_scope(name):
            return run(*args)

    early = slots // 4
    step("w_feat", fetch(0).wait)
    step("barrier", pl.semaphore_wait, barrier, jnp.where(outer, 5, 6))
    step("own0", gather_own, 0)
    step("tables", tables)
    table_copy.start()
    step("prepare", prepare)
    step("loads", wait_loads)
    step("forward0a", forward, 0, 0)
    running = step("merge0", merge_slots, 0, early, jnp.zeros((tile, tile), merged.dtype))
    step("forward0b", forward, 0, 1)
    step("own1", gather_own, 1)
    step("merge1", merge_slots, early, slots, running)
    step("share_near0", share_near, 0)
    step("pair0a0", add_pair, 0, (0, 1), 0, one)
    step("pair0a1", add_pair, 0, (0, 1), 1, one)
    step("share_far0", share_far, 0)
    step("w_x0", wait_for, 0, SIB_XY)
    step("pair0x0", add_pair, 0, (2, 3), 0, one)
    step("pair0y0", add_pair, 0, (4, 5), 0, one)
    step("w_d0", wait_for, 0, SIB_D)
    step("last00", last_pair, 0, 0)
    step("forward1a", forward, 1, 0)
    step("pair0x1", add_pair, 0, (2, 3), 1, one)
    step("forward1b", forward, 1, 1)
    step("pair0y1", add_pair, 0, (4, 5), 1, one)
    step("last01", last_pair, 0, 1)
    step("share_near1", share_near, 1)
    step("near_seg0", near_first)
    step("relay000", relay_sum, 0, 0, 0)
    step("pair1a", add_pair, 1, (0, 1), 0, 2)
    step("share_far1", share_far, 1)
    step("w_x1", wait_for, 1, SIB_XY)
    step("pair1x", add_pair, 1, (2, 3), 0, 2)
    step("relay001", relay_sum, 0, 0, 1)
    step("pair1y", add_pair, 1, (4, 5), 0, 2)
    step("relay010", relay_sum, 0, 1, 0)
    step("w_d1", wait_for, 1, SIB_D)
    step("near_seg1i", near_segment, jnp.logical_not(outer))
    step("relay011", relay_sum, 0, 1, 1)
    step("last10", last_pair, 1, 0)
    step("last11", last_pair, 1, 1)
    near_rest()
    step("near_seg1o", near_segment, outer)
    for i in range(2):
        for q in range(PIECES[1]):
            step(f"relay1{i}{q}", relay_sum, 1, i, q)
    step("own_seg", own_segment)
    step("finish", finish)
    step("drain", drain)


def local_fused(n_row, n_col, features, in_degree, tile_index, tile_count, adjacency_tiles, projection, out_bias):
    seg, width = features.shape
    slots, tile, _ = adjacency_tiles.shape
    halves = width // LANES
    positions = (seg * n_col // tile) * (seg * n_row // tile)
    lines = 2 * (slots // LANES) + positions // LANES
    hbm = pl.BlockSpec(memory_space=pltpu.HBM)
    args = [features, tile_index.T, tile_count, adjacency_tiles,
            in_degree.reshape(seg // LANES, LANES), projection, out_bias[None, :]]
    specs = [hbm] * len(args)
    specs[2] = pl.BlockSpec(memory_space=pltpu.SMEM)
    args = [a if i == 2 else pltpu.with_memory_space_constraint(a, pltpu.HBM) for i, a in enumerate(args)]
    return pl.pallas_call(
        fused_kernel,
        out_shape=jax.ShapeDtypeStruct((seg, projection.shape[1]), jnp.bfloat16),
        in_specs=specs,
        out_specs=pl.BlockSpec(memory_space=pltpu.VMEM),
        scratch_shapes=[
            pltpu.VMEM(features.shape, features.dtype),
            pltpu.VMEM((2, slots), jnp.int32),
            pltpu.VMEM((seg // LANES, LANES), jnp.int32),
            pltpu.VMEM(projection.shape, projection.dtype),
            pltpu.VMEM((1, projection.shape[1]), jnp.float32),
            pltpu.VMEM((slots, tile, tile), jnp.bfloat16),
            pltpu.VMEM((slots + 1, tile, tile), jnp.bfloat16),
            pltpu.VMEM((lines, LANES), jnp.int32),
            pltpu.SMEM((lines, LANES), jnp.int32),
            pltpu.VMEM((halves, n_row, seg, LANES), jnp.bfloat16),
            pltpu.VMEM((halves, 2, seg, LANES), jnp.float32),
            pltpu.VMEM((seg, width), jnp.float32),
            pltpu.VMEM((seg, projection.shape[1]), jnp.float32),
            pltpu.VMEM((seg, LANES), jnp.float32),
            pltpu.VMEM((halves, 2, seg, LANES), jnp.bfloat16),
            pltpu.VMEM((halves, seg, LANES), jnp.bfloat16),
            pltpu.VMEM((halves, 2, seg, LANES), jnp.bfloat16),
            pltpu.VMEM((halves, seg, LANES), jnp.bfloat16),
            pltpu.VMEM((halves, seg, LANES), jnp.bfloat16),
            pltpu.SemaphoreType.DMA((len(args) - 2,)),
            pltpu.SemaphoreType.DMA,
            pltpu.SemaphoreType.DMA,
            pltpu.SemaphoreType.DMA,
            pltpu.SemaphoreType.DMA((halves, ARRIVALS)),
            pltpu.SemaphoreType.DMA((2 * sum(PIECES),)),
            pltpu.SemaphoreType.DMA((1 + PIECES[1],)),
            pltpu.SemaphoreType.DMA((1 + NEAR[1],)),
        ],
        compiler_params=pltpu.CompilerParams(
            collective_id=0, has_side_effects=True, vmem_limit_bytes=48 * 1024 * 1024),
    )(*args)


def solution(mesh):
    n_row, n_col = mesh.shape["row"], mesh.shape["col"]

    def local(features, in_degree, tile_index, tile_count, adjacency_tiles, projection, out_bias):
        seg, width = features.shape
        slots, tile, _ = adjacency_tiles.shape
        positions = (seg * n_col // LANES) * (seg * n_row // LANES)
        fits = (
            n_row == 8 and n_col == 4 and tile == LANES and slots <= 256 and slots % LANES == 0
            and 4 * slots * tile * tile <= MERGE_LIMIT
            and seg % (4 * LANES) == 0 and width == 2 * LANES and positions % LANES == 0
            and LANES % (positions // n_row) == 0)
        args = (features, in_degree, tile_index, tile_count, adjacency_tiles, projection, out_bias)
        return local_fused(n_row, n_col, *args) if fits else local_sparse(*args)

    return jax.shard_map(
        local,
        mesh=mesh,
        in_specs=(
            P(("row", "col"), None),
            P(("row", "col")),
            P(("row", "col"), None),
            P(("row", "col")),
            P(("row", "col"), None, None),
            P(),
            P(),
        ),
        out_specs=P(("row", "col"), None),
        check_vma=False,
    )
```

```python
import functools

import jax
import jax.numpy as jnp
from jax import lax
from jax.experimental import pallas as pl
from jax.experimental.pallas import tpu as pltpu
from jax.sharding import PartitionSpec as P

BLK = 32
LANES = 128
CHUNKS = 16
PIECES = (2, 4)
NEAR = (2, 4)
ARRIVALS = 6
X, Y = 3, 5
UNROLL = 8
MERGE_LIMIT = 20 * 1024 * 1024
MESH = pl.DeviceIdType.MESH


def block_terms(running, col_blocks, index_block, tile_block, live_block):
    picked = col_blocks[index_block[:, 1]]
    kept = jnp.where(live_block[:, None, None], tile_block, jnp.zeros_like(tile_block))
    product = jnp.einsum("kij,kjf->kif", kept, picked, preferred_element_type=jnp.float32)
    flattened = product.reshape(product.shape[0], -1)
    return running.at[index_block[:, 0]].add(flattened)


def local_sparse(features, in_degree, tile_index, tile_count, adjacency_tiles, projection, out_bias):
    feat_width = features.shape[1]
    tile_size = adjacency_tiles.shape[1]
    slot_total = adjacency_tiles.shape[0]
    gathered = lax.all_gather(features, "row", axis=0, tiled=True)
    col_blocks = gathered.reshape(gathered.shape[0] // tile_size, tile_size, feat_width)
    row_blocks = features.shape[0] * lax.axis_size("col") // tile_size
    live_count = tile_count[0]
    zeroed = jnp.zeros((row_blocks, tile_size * feat_width), jnp.float32)

    def one_step(running, offset):
        index_block = lax.dynamic_slice_in_dim(tile_index, offset, BLK, 0)
        tile_block = lax.dynamic_slice_in_dim(adjacency_tiles, offset, BLK, 0)
        live_block = offset + jnp.arange(BLK, dtype=jnp.int32) < live_count
        return (block_terms(running, col_blocks, index_block, tile_block, live_block), None)

    summed, _ = lax.scan(one_step, zeroed, jnp.arange(0, slot_total, BLK, dtype=jnp.int32))
    partial_value = summed.reshape(row_blocks * tile_size, feat_width)
    own_sums = lax.psum_scatter(partial_value, "col", scatter_dimension=0, tiled=True)
    neighbour_mean = (own_sums / in_degree[:, None].astype(jnp.float32)).astype(jnp.bfloat16)
    joined = jnp.concatenate([features, neighbour_mean], axis=1)
    mixed = jnp.dot(joined, projection, preferred_element_type=jnp.float32) + out_bias[None, :]
    return jnp.maximum(mixed, 0.0).astype(jnp.bfloat16)


def slot_tables(place_ref, count, table_ref, row_blocks, positions):
    slots = place_ref.shape[1]
    chunks = slots // LANES
    slot_row = lax.broadcasted_iota(jnp.int32, (1, slots), 1)
    spot_row = place_ref[1:2, :] * row_blocks + place_ref[0:1, :]
    spot_row = jnp.where(slot_row < count, spot_row, positions)

    def lane(v, i):
        return v[:, i * LANES:(i + 1) * LANES]

    spot = jnp.concatenate(
        [jnp.transpose(jnp.broadcast_to(lane(spot_row, i), (LANES, LANES))) for i in range(chunks)], axis=0)
    slot = lax.broadcasted_iota(jnp.int32, (slots, LANES), 0)
    before = jnp.zeros((slots, LANES), jnp.float32)
    repeat = jnp.zeros((slots, LANES), jnp.float32)
    for i in range(chunks):
        equal = lane(spot_row, i) == spot
        earlier = lane(slot_row, i) < slot
        first = (lane(spot_row, i) < spot) | (equal & earlier)
        before = before + jnp.where(first, 1.0, 0.0)
        repeat = jnp.maximum(repeat, jnp.where(equal & earlier, 1.0, 0.0))
    rank = jnp.sum(before, axis=1, keepdims=True).astype(jnp.int32)
    keep = jnp.max(repeat, axis=1, keepdims=True)
    for i in range(chunks):
        hit = rank == lax.broadcasted_iota(jnp.int32, (slots, LANES), 1) + i * LANES
        order = jnp.sum(jnp.where(hit, slot, 0), axis=0, keepdims=True)
        again = jnp.sum(jnp.where(hit, keep, 0.0), axis=0, keepdims=True)
        table_ref[i:i + 1, :] = order
        table_ref[chunks + i:chunks + i + 1, :] = again.astype(jnp.int32)
    for i in range(positions // LANES):
        here = lax.broadcasted_iota(jnp.int32, (slots, LANES), 1) + i * LANES
        upto = jnp.sum(jnp.where(spot <= here, 1, 0), axis=0, keepdims=True)
        count_here = jnp.sum(jnp.where(spot == here, 1, 0), axis=0, keepdims=True)
        table_ref[2 * chunks + i:2 * chunks + i + 1, :] = jnp.where(count_here > 0, upto - 1, slots)


def fused_kernel(feat_hbm, place_hbm, count_ref, tiles_ref, degree_hbm, proj_hbm, bias_hbm, out_ref,
                 feat_ref, place_ref, degree_ref, proj_ref, bias_ref,
                 stage, merged, table_v, table, gathered, acc, own, hidden, degree_col,
                 send, send_near, relayed, far, near_in,
                 in_sem, tile_sem, table_sem, sent, ag_recv, relay_sem, far_sem, near_sem, inner_ready):
    seg, width = feat_ref.shape
    slots, tile, _ = stage.shape
    halves = width // LANES
    blocks = seg // tile
    n_row, n_col = gathered.shape[1], 4
    row_blocks = n_col * blocks
    positions = blocks * n_row * row_blocks
    half_rows, quarter = seg // 2, seg // 4
    per = slots // CHUNKS
    r = lax.axis_index("row")
    c = lax.axis_index("col")
    one = c // n_col + 1
    near = c ^ 1
    upper = c < 2
    outer = (c == 0) | (c == 3)
    dests = (jnp.where(upper, 3, 0), jnp.where(upper, 2, 1), near, c)

    inputs = [(place_hbm, place_ref), (degree_hbm, degree_ref), (proj_hbm, proj_ref), (bias_hbm, bias_ref)]

    def lanes(h):
        return pl.ds(h * LANES, LANES)

    def fetch(i):
        return pltpu.make_async_copy(*inputs[i], in_sem.at[halves + i])

    def fetch_features(h, rows):
        return pltpu.make_async_copy(feat_hbm.at[rows, lanes(h)], feat_ref.at[rows, lanes(h)], in_sem.at[h])

    rows_of = [pl.ds(i * quarter, quarter) for i in range(4)]
    whole = pl.ds(0, seg)
    for rows in rows_of:
        fetch_features(0, rows).start()
    fetch(0).start()
    for h in range(1, halves):
        fetch_features(h, whole).start()

    barrier = pltpu.get_barrier_semaphore()

    def greet(row, col):
        pl.semaphore_signal(barrier, inc=1, device_id=(row, col), device_id_type=MESH)

    for m in (1, X, Y):
        greet(r ^ m, c)

    @pl.when(outer)
    def _():
        greet(r, near)
        greet(r, c ^ 2)

    @pl.when(jnp.logical_not(outer))
    def _():
        greet(r, c ^ 3)

    for i in range(1, len(inputs)):
        fetch(i).start()
    for i in range(CHUNKS):
        part = pl.ds(i * per, per)
        pltpu.make_async_copy(tiles_ref.at[part], stage.at[part], tile_sem).start()

    first_rows, last_rows = pl.ds(0, half_rows), pl.ds(half_rows, half_rows)
    FROM_1, FROM_2, FROM_3, FROM_FAR, SIB_XY, SIB_D = range(ARRIVALS)
    arriving_rows = (half_rows, half_rows, 2 * seg, seg, 2 * seg, seg)

    def gather_start(h, flip, rows, step, arrival):
        owner = r ^ flip
        src = feat_ref.at[rows, lanes(h)] if flip == 0 else gathered.at[h, owner, rows, :]
        pltpu.make_async_remote_copy(
            src_ref=src, dst_ref=gathered.at[h, owner, rows, :],
            send_sem=sent, recv_sem=ag_recv.at[h, arrival],
            device_id=(r ^ step, c), device_id_type=MESH).start()

    def wait_for(h, arrival):
        rows = arriving_rows[arrival]
        if rows <= seg:
            ref = gathered.at[h, 0, pl.ds(0, rows), :]
        else:
            ref = gathered.at[h, pl.ds(0, rows // seg)]
        pltpu.make_async_remote_copy(
            src_ref=ref, dst_ref=ref,
            send_sem=sent, recv_sem=ag_recv.at[h, arrival],
            device_id=(r ^ 1, c), device_id_type=MESH).wait_recv()

    def gather_own(h):
        gather_start(h, 0, rows_of[0], X, FROM_1)
        gather_start(h, 0, rows_of[2], Y, FROM_1)
        gather_start(h, 0, rows_of[1], X, FROM_2)
        gather_start(h, 0, rows_of[3], Y, FROM_2)
        gather_start(h, 0, last_rows, X, FROM_3)
        gather_start(h, 0, first_rows, Y, FROM_3)

    def gather_sibling(h):
        gather_start(h, 0, whole, 1, FROM_3)

    def forward(h, part):
        wait_for(h, (FROM_1, FROM_2)[part])
        gather_start(h, X, rows_of[part], Y, FROM_FAR)
        gather_start(h, Y, rows_of[2 + part], X, FROM_FAR)

    def share_near(h):
        wait_for(h, FROM_3)
        gather_start(h, X, whole, 1, SIB_XY)
        gather_start(h, Y, whole, 1, SIB_XY)

    def share_far(h):
        wait_for(h, FROM_FAR)
        gather_start(h, 6, whole, 1, SIB_D)

    def block_of(h, flip):
        if h is None:
            return jnp.concatenate([block_of(i, flip) for i in range(halves)], axis=1)
        return feat_ref[:, lanes(h)] if flip == 0 else gathered[h, r ^ flip]

    def product(h, flips, dest, group=None):
        columns = []
        for flip in flips:
            base = (r ^ flip) * (blocks * row_blocks)
            line = 2 * (slots // LANES) + base // LANES
            spot = base % LANES + dest * blocks
            columns += [(line, spot + k * row_blocks) for k in range(blocks)]
        picks = range(blocks) if group is None else [group * (blocks // 2) + k for k in range(blocks // 2)]
        left = jnp.concatenate(
            [jnp.concatenate([merged[table[line, spot + b]] for line, spot in columns], axis=1)
             for b in picks], axis=0)
        right = jnp.concatenate([block_of(h, flip) for flip in flips], axis=0)
        return jnp.dot(left, right, preferred_element_type=jnp.float32)

    def half_of(g):
        return pl.ds(pl.multiple_of(g * half_rows, half_rows), half_rows)

    def add_pair(h, flips, low, count):
        @pl.loop(low, low + count)
        def _(i):
            dest = jnp.where(i == 0, dests[0], dests[1])
            if flips[0] == 0:
                acc[h, i] = product(h, flips, dest)
            else:
                acc[h, i] += product(h, flips, dest)

    def piece(q, pieces):
        size = seg // pieces
        return pl.ds(pl.multiple_of(q * size, size), size)

    def sum_copy(src, dst, recv, row, col):
        return pltpu.make_async_remote_copy(
            src_ref=src, dst_ref=dst, send_sem=sent, recv_sem=recv,
            device_id=(row, col), device_id_type=MESH)

    def relay_copy(h, i, q):
        rows = piece(q, PIECES[h])
        return sum_copy(send.at[h, i, rows, :], relayed.at[h, i, rows, :],
                        relay_sem.at[2 * sum(PIECES[:h]) + i * PIECES[h] + q], r, near)

    def far_copy(h, i, q):
        rows = piece(q, PIECES[h])
        return sum_copy(send.at[h, i, rows, :], far.at[h, rows, :],
                        far_sem.at[0 if h == 0 else q + 1], r, dests[i])

    def near_copy(h, q):
        rows = piece(q, NEAR[h])
        return sum_copy(send_near.at[h, rows, :], near_in.at[h, rows, :],
                        near_sem.at[0 if h == 0 else q + 1], r, near)

    def last_pair(h, i):
        each = PIECES[h] // 2

        @pl.loop(0, 2)
        def _(g):
            rows = half_of(g)
            total = acc[h, i, rows, :] + product(h, (6, 7), dests[i], g)
            acc[h, i, rows, :] = total

            @pl.when(outer)
            def _():
                send[h, i, rows, :] = total.astype(send.dtype)
                for k in range(each):
                    relay_copy(h, i, g * each + k).start()

    def relay_sum(h, i, q):
        @pl.when(jnp.logical_not(outer))
        def _():
            rows = piece(q, PIECES[h])
            relay_copy(h, i, q).wait_recv()
            total = acc[h, i, rows, :] + relayed[h, i, rows, :].astype(jnp.float32)
            send[h, i, rows, :] = total.astype(send.dtype)
            far_copy(h, i, q).start()

    def tell_outer():
        @pl.when(jnp.logical_not(outer))
        def _():
            for col in (near, c ^ 2):
                pl.semaphore_signal(inner_ready, inc=1, device_id=(r, col), device_id_type=MESH)

    def hear_inner():
        @pl.when(outer)
        def _():
            pl.semaphore_wait(inner_ready, 2)

    def near_product(h, trips):
        @pl.loop(0, trips)
        def _(g):
            rows = half_of(g)
            send_near[h, rows, :] = product(h, range(n_row), near, g).astype(send_near.dtype)

    def near_segment(mine):
        near_product(1, jnp.where(mine, 2, 0))

        @pl.when(mine)
        def _():
            for q in range(NEAR[1]):
                near_copy(1, q).start()

    def near_first():
        near_product(0, 2)
        near_copy(0, 0).start()

        @pl.when(jnp.logical_not(outer))
        def _():
            near_copy(0, 1).start()

    def near_rest():
        @pl.when(outer)
        def _():
            near_copy(0, 1).start()

    def own_segment():
        @pl.loop(0, 2)
        def _(g):
            own[half_of(g), :] = product(None, range(n_row), c, g)

    def finish():
        sum_copy(far.at[0], far.at[0], far_sem.at[0], r, near).wait_recv()
        sum_copy(near_in.at[0], near_in.at[0], near_sem.at[0], r, near).wait_recv()
        pieces = NEAR[1]
        for q in range(pieces):
            rows = piece(q, pieces)
            far_copy(1, 0, q).wait_recv()
            near_copy(1, q).wait_recv()
            divisor = degree_col[rows, :]
            mean = jnp.concatenate(
                [((own[rows, lanes(h)] + far[h, rows, :].astype(jnp.float32)
                   + near_in[h, rows, :].astype(jnp.float32)) / divisor).astype(jnp.bfloat16)
                 for h in range(halves)], axis=1)
            mixed = hidden[rows, :] + jnp.dot(
                mean, proj_ref[width:, :], preferred_element_type=jnp.float32)
            out_ref[rows, :] = jnp.maximum(mixed, 0.0).astype(out_ref.dtype)

    def tables():
        fetch(0).wait()
        merged[slots] = jnp.zeros((tile, tile), merged.dtype)
        slot_tables(place_ref, count_ref[0], table_v, row_blocks, positions)

    table_copy = pltpu.make_async_copy(table_v, table, table_sem)

    def wait_loads():
        table_copy.wait()
        pltpu.make_async_copy(tiles_ref, stage, tile_sem).wait()

    def merge_slots(low, high, running):
        for part in range(slots // LANES):
            def merge(i, running, part=part):
                keep = table[slots // LANES + part, i].astype(jnp.float32)
                kept = jnp.broadcast_to(keep, (16, tile)).astype(running.dtype)
                kept = jnp.concatenate([kept] * (tile // 16), axis=0)
                running = stage[table[part, i]] + running * kept
                merged[part * LANES + i] = running
                return running
            begin, end = max(low - part * LANES, 0), min(high - part * LANES, LANES)
            if begin < end:
                running = lax.fori_loop(begin, end, merge, running, unroll=UNROLL)
        return running

    def prepare():
        for h in range(1, halves):
            fetch_features(h, whole).wait()
        for i in range(1, len(inputs)):
            fetch(i).wait()
        hidden[...] = jnp.dot(
            feat_ref[...], proj_ref[:width, :], preferred_element_type=jnp.float32) + bias_ref[...]
        for b in range(seg // LANES):
            one = degree_ref[b:b + 1, :].astype(jnp.float32)
            degree_col[b * LANES:(b + 1) * LANES, :] = jnp.transpose(jnp.broadcast_to(one, (LANES, LANES)))

    def drain():
        tiles_sent = halves * 10 * seg * LANES // (tile * tile)
        sum_copy(stage.at[pl.ds(0, tiles_sent)], stage.at[pl.ds(0, tiles_sent)],
                 near_sem.at[0], r, near).wait_send()

    def step(name, run, *args):
        with jax.named_scope(name):
            return run(*args)

    early = slots // 4
    step("w_feat", fetch_features(0, whole).wait)
    step("barrier", pl.semaphore_wait, barrier, jnp.where(outer, 3, 6))
    step("own0", gather_own, 0)
    gather_sibling(0)
    tell_outer()
    step("tables", tables)
    table_copy.start()
    step("prepare", prepare)
    step("loads", wait_loads)
    step("forward0a", forward, 0, 0)
    running = step("merge0", merge_slots, 0, early, jnp.zeros((tile, tile), merged.dtype))
    step("forward0b", forward, 0, 1)
    step("merge1", merge_slots, early, slots, running)
    step("share_near0", share_near, 0)
    step("pair0a0", add_pair, 0, (0, 1), 0, one)
    step("pair0a1", add_pair, 0, (0, 1), 1, one)
    step("share_far0", share_far, 0)
    step("own1", gather_own, 1)
    gather_sibling(1)
    step("w_x0", wait_for, 0, SIB_XY)
    step("pair0x0", add_pair, 0, (2, 3), 0, one)
    step("pair0y0", add_pair, 0, (4, 5), 0, one)
    step("w_d0", wait_for, 0, SIB_D)
    hear_inner()
    step("last00", last_pair, 0, 0)
    step("pair0x1", add_pair, 0, (2, 3), 1, one)
    step("pair0y1", add_pair, 0, (4, 5), 1, one)
    step("last01", last_pair, 0, 1)
    step("forward1a", forward, 1, 0)
    step("forward1b", forward, 1, 1)
    step("near_seg0", near_first)
    step("share_near1", share_near, 1)
    step("relay000", relay_sum, 0, 0, 0)
    step("pair1a", add_pair, 1, (0, 1), 0, 2)
    step("w_x1", wait_for, 1, SIB_XY)
    step("pair1x", add_pair, 1, (2, 3), 0, 2)
    step("share_far1", share_far, 1)
    step("relay001", relay_sum, 0, 0, 1)
    step("pair1y", add_pair, 1, (4, 5), 0, 2)
    step("relay010", relay_sum, 0, 1, 0)
    step("w_d1", wait_for, 1, SIB_D)
    step("near_seg1i", near_segment, jnp.logical_not(outer))
    step("relay011", relay_sum, 0, 1, 1)
    step("last10", last_pair, 1, 0)
    step("last11", last_pair, 1, 1)
    near_rest()
    step("near_seg1o", near_segment, outer)
    for i in range(2):
        for q in range(PIECES[1]):
            step(f"relay1{i}{q}", relay_sum, 1, i, q)
    step("own_seg", own_segment)
    step("finish", finish)
    step("drain", drain)


def local_fused(n_row, n_col, features, in_degree, tile_index, tile_count, adjacency_tiles, projection, out_bias):
    seg, width = features.shape
    slots, tile, _ = adjacency_tiles.shape
    halves = width // LANES
    positions = (seg * n_col // tile) * (seg * n_row // tile)
    lines = 2 * (slots // LANES) + positions // LANES
    hbm = pl.BlockSpec(memory_space=pltpu.HBM)
    args = [features, tile_index.T, tile_count, adjacency_tiles,
            in_degree.reshape(seg // LANES, LANES), projection, out_bias[None, :]]
    specs = [hbm] * len(args)
    specs[2] = pl.BlockSpec(memory_space=pltpu.SMEM)
    args = [a if i == 2 else pltpu.with_memory_space_constraint(a, pltpu.HBM) for i, a in enumerate(args)]
    return pl.pallas_call(
        fused_kernel,
        out_shape=jax.ShapeDtypeStruct((seg, projection.shape[1]), jnp.bfloat16),
        in_specs=specs,
        out_specs=pl.BlockSpec(memory_space=pltpu.VMEM),
        scratch_shapes=[
            pltpu.VMEM(features.shape, features.dtype),
            pltpu.VMEM((2, slots), jnp.int32),
            pltpu.VMEM((seg // LANES, LANES), jnp.int32),
            pltpu.VMEM(projection.shape, projection.dtype),
            pltpu.VMEM((1, projection.shape[1]), jnp.float32),
            pltpu.VMEM((slots, tile, tile), jnp.bfloat16),
            pltpu.VMEM((slots + 1, tile, tile), jnp.bfloat16),
            pltpu.VMEM((lines, LANES), jnp.int32),
            pltpu.SMEM((lines, LANES), jnp.int32),
            pltpu.VMEM((halves, n_row, seg, LANES), jnp.bfloat16),
            pltpu.VMEM((halves, 2, seg, LANES), jnp.float32),
            pltpu.VMEM((seg, width), jnp.float32),
            pltpu.VMEM((seg, projection.shape[1]), jnp.float32),
            pltpu.VMEM((seg, LANES), jnp.float32),
            pltpu.VMEM((halves, 2, seg, LANES), jnp.bfloat16),
            pltpu.VMEM((halves, seg, LANES), jnp.bfloat16),
            pltpu.VMEM((halves, 2, seg, LANES), jnp.bfloat16),
            pltpu.VMEM((halves, seg, LANES), jnp.bfloat16),
            pltpu.VMEM((halves, seg, LANES), jnp.bfloat16),
            pltpu.SemaphoreType.DMA((halves + len(args) - 3,)),
            pltpu.SemaphoreType.DMA,
            pltpu.SemaphoreType.DMA,
            pltpu.SemaphoreType.DMA,
            pltpu.SemaphoreType.DMA((halves, ARRIVALS)),
            pltpu.SemaphoreType.DMA((2 * sum(PIECES),)),
            pltpu.SemaphoreType.DMA((1 + PIECES[1],)),
            pltpu.SemaphoreType.DMA((1 + NEAR[1],)),
            pltpu.SemaphoreType.REGULAR,
        ],
        compiler_params=pltpu.CompilerParams(
            collective_id=0, has_side_effects=True, vmem_limit_bytes=48 * 1024 * 1024),
    )(*args)


def solution(mesh):
    n_row, n_col = mesh.shape["row"], mesh.shape["col"]

    def local(features, in_degree, tile_index, tile_count, adjacency_tiles, projection, out_bias):
        seg, width = features.shape
        slots, tile, _ = adjacency_tiles.shape
        positions = (seg * n_col // LANES) * (seg * n_row // LANES)
        fits = (
            n_row == 8 and n_col == 4 and tile == LANES and slots <= 256 and slots % LANES == 0
            and 4 * slots * tile * tile <= MERGE_LIMIT
            and seg % (4 * LANES) == 0 and width == 2 * LANES and positions % LANES == 0
            and LANES % (positions // n_row) == 0)
        args = (features, in_degree, tile_index, tile_count, adjacency_tiles, projection, out_bias)
        return local_fused(n_row, n_col, *args) if fits else local_sparse(*args)

    return jax.shard_map(
        local,
        mesh=mesh,
        in_specs=(
            P(("row", "col"), None),
            P(("row", "col")),
            P(("row", "col"), None),
            P(("row", "col")),
            P(("row", "col"), None, None),
            P(),
            P(),
        ),
        out_specs=P(("row", "col"), None),
        check_vma=False,
    )
```

```python
import functools

import jax
import jax.numpy as jnp
from jax import lax
from jax.experimental import pallas as pl
from jax.experimental.pallas import tpu as pltpu
from jax.sharding import PartitionSpec as P

BLK = 32
LANES = 128
CHUNKS = 16
PIECES = (2, 4)
NEAR = (2, 4)
ARRIVALS = 6
X, Y = 3, 5
UNROLL = 8
MERGE_LIMIT = 20 * 1024 * 1024
MESH = pl.DeviceIdType.MESH


def block_terms(running, col_blocks, index_block, tile_block, live_block):
    picked = col_blocks[index_block[:, 1]]
    kept = jnp.where(live_block[:, None, None], tile_block, jnp.zeros_like(tile_block))
    product = jnp.einsum("kij,kjf->kif", kept, picked, preferred_element_type=jnp.float32)
    flattened = product.reshape(product.shape[0], -1)
    return running.at[index_block[:, 0]].add(flattened)


def local_sparse(features, in_degree, tile_index, tile_count, adjacency_tiles, projection, out_bias):
    feat_width = features.shape[1]
    tile_size = adjacency_tiles.shape[1]
    slot_total = adjacency_tiles.shape[0]
    gathered = lax.all_gather(features, "row", axis=0, tiled=True)
    col_blocks = gathered.reshape(gathered.shape[0] // tile_size, tile_size, feat_width)
    row_blocks = features.shape[0] * lax.axis_size("col") // tile_size
    live_count = tile_count[0]
    zeroed = jnp.zeros((row_blocks, tile_size * feat_width), jnp.float32)

    def one_step(running, offset):
        index_block = lax.dynamic_slice_in_dim(tile_index, offset, BLK, 0)
        tile_block = lax.dynamic_slice_in_dim(adjacency_tiles, offset, BLK, 0)
        live_block = offset + jnp.arange(BLK, dtype=jnp.int32) < live_count
        return (block_terms(running, col_blocks, index_block, tile_block, live_block), None)

    summed, _ = lax.scan(one_step, zeroed, jnp.arange(0, slot_total, BLK, dtype=jnp.int32))
    partial_value = summed.reshape(row_blocks * tile_size, feat_width)
    own_sums = lax.psum_scatter(partial_value, "col", scatter_dimension=0, tiled=True)
    neighbour_mean = (own_sums / in_degree[:, None].astype(jnp.float32)).astype(jnp.bfloat16)
    joined = jnp.concatenate([features, neighbour_mean], axis=1)
    mixed = jnp.dot(joined, projection, preferred_element_type=jnp.float32) + out_bias[None, :]
    return jnp.maximum(mixed, 0.0).astype(jnp.bfloat16)


def slot_tables(place_ref, count, table_ref, row_blocks, positions):
    slots = place_ref.shape[1]
    chunks = slots // LANES
    slot_row = lax.broadcasted_iota(jnp.int32, (1, slots), 1)
    spot_row = place_ref[1:2, :] * row_blocks + place_ref[0:1, :]
    spot_row = jnp.where(slot_row < count, spot_row, positions)

    def lane(v, i):
        return v[:, i * LANES:(i + 1) * LANES]

    spot = jnp.concatenate(
        [jnp.transpose(jnp.broadcast_to(lane(spot_row, i), (LANES, LANES))) for i in range(chunks)], axis=0)
    slot = lax.broadcasted_iota(jnp.int32, (slots, LANES), 0)
    before = jnp.zeros((slots, LANES), jnp.float32)
    repeat = jnp.zeros((slots, LANES), jnp.float32)
    for i in range(chunks):
        equal = lane(spot_row, i) == spot
        earlier = lane(slot_row, i) < slot
        first = (lane(spot_row, i) < spot) | (equal & earlier)
        before = before + jnp.where(first, 1.0, 0.0)
        repeat = jnp.maximum(repeat, jnp.where(equal & earlier, 1.0, 0.0))
    rank = jnp.sum(before, axis=1, keepdims=True).astype(jnp.int32)
    keep = jnp.max(repeat, axis=1, keepdims=True)
    for i in range(chunks):
        hit = rank == lax.broadcasted_iota(jnp.int32, (slots, LANES), 1) + i * LANES
        order = jnp.sum(jnp.where(hit, slot, 0), axis=0, keepdims=True)
        again = jnp.sum(jnp.where(hit, keep, 0.0), axis=0, keepdims=True)
        table_ref[i:i + 1, :] = order
        table_ref[chunks + i:chunks + i + 1, :] = again.astype(jnp.int32)
    for i in range(positions // LANES):
        here = lax.broadcasted_iota(jnp.int32, (slots, LANES), 1) + i * LANES
        upto = jnp.sum(jnp.where(spot <= here, 1, 0), axis=0, keepdims=True)
        count_here = jnp.sum(jnp.where(spot == here, 1, 0), axis=0, keepdims=True)
        table_ref[2 * chunks + i:2 * chunks + i + 1, :] = jnp.where(count_here > 0, upto - 1, slots)


def fused_kernel(feat_hbm, place_hbm, count_ref, tiles_ref, degree_hbm, proj_hbm, bias_hbm, out_ref,
                 feat_ref, place_ref, degree_ref, proj_ref, bias_ref,
                 stage, merged, table_v, table, gathered, acc, own, hidden, degree_col,
                 send, send_near, relayed, far, near_in,
                 in_sem, tile_sem, table_sem, sent, ag_recv, relay_sem, far_sem, near_sem, inner_ready):
    seg, width = feat_ref.shape
    slots, tile, _ = stage.shape
    halves = width // LANES
    blocks = seg // tile
    n_row, n_col = gathered.shape[1], 4
    row_blocks = n_col * blocks
    positions = blocks * n_row * row_blocks
    half_rows, quarter = seg // 2, seg // 4
    per = slots // CHUNKS
    r = lax.axis_index("row")
    c = lax.axis_index("col")
    one = c // n_col + 1
    near = c ^ 1
    upper = c < 2
    outer = (c == 0) | (c == 3)
    dests = (jnp.where(upper, 3, 0), jnp.where(upper, 2, 1), near, c)

    inputs = [(place_hbm, place_ref), (degree_hbm, degree_ref), (proj_hbm, proj_ref), (bias_hbm, bias_ref)]

    def lanes(h):
        return pl.ds(h * LANES, LANES)

    def fetch(i):
        return pltpu.make_async_copy(*inputs[i], in_sem.at[halves + i])

    def fetch_features(h, rows):
        return pltpu.make_async_copy(feat_hbm.at[rows, lanes(h)], feat_ref.at[rows, lanes(h)], in_sem.at[h])

    rows_of = [pl.ds(i * quarter, quarter) for i in range(4)]
    whole = pl.ds(0, seg)
    for rows in rows_of:
        fetch_features(0, rows).start()
    fetch(0).start()
    for h in range(1, halves):
        fetch_features(h, whole).start()

    barrier = pltpu.get_barrier_semaphore()

    def greet(row, col):
        pl.semaphore_signal(barrier, inc=1, device_id=(row, col), device_id_type=MESH)

    for m in (1, X, Y):
        greet(r ^ m, c)

    @pl.when(outer)
    def _():
        greet(r, near)
        greet(r, c ^ 2)

    @pl.when(jnp.logical_not(outer))
    def _():
        greet(r, c ^ 3)

    for i in range(1, len(inputs)):
        fetch(i).start()
    for i in range(CHUNKS):
        part = pl.ds(i * per, per)
        pltpu.make_async_copy(tiles_ref.at[part], stage.at[part], tile_sem).start()

    first_rows, last_rows = pl.ds(0, half_rows), pl.ds(half_rows, half_rows)
    FROM_1, FROM_2, FROM_3, FROM_FAR, SIB_XY, SIB_D = range(ARRIVALS)
    arriving_rows = (half_rows, half_rows, 2 * seg, seg, 2 * seg, seg)

    def gather_start(h, flip, rows, step, arrival):
        owner = r ^ flip
        src = feat_ref.at[rows, lanes(h)] if flip == 0 else gathered.at[h, owner, rows, :]
        pltpu.make_async_remote_copy(
            src_ref=src, dst_ref=gathered.at[h, owner, rows, :],
            send_sem=sent, recv_sem=ag_recv.at[h, arrival],
            device_id=(r ^ step, c), device_id_type=MESH).start()

    def wait_for(h, arrival):
        rows = arriving_rows[arrival]
        if rows <= seg:
            ref = gathered.at[h, 0, pl.ds(0, rows), :]
        else:
            ref = gathered.at[h, pl.ds(0, rows // seg)]
        pltpu.make_async_remote_copy(
            src_ref=ref, dst_ref=ref,
            send_sem=sent, recv_sem=ag_recv.at[h, arrival],
            device_id=(r ^ 1, c), device_id_type=MESH).wait_recv()

    def gather_own(h):
        gather_start(h, 0, rows_of[0], X, FROM_1)
        gather_start(h, 0, rows_of[2], Y, FROM_1)
        gather_start(h, 0, rows_of[1], X, FROM_2)
        gather_start(h, 0, rows_of[3], Y, FROM_2)
        gather_start(h, 0, last_rows, X, FROM_3)
        gather_start(h, 0, first_rows, Y, FROM_3)

    def gather_sibling(h):
        gather_start(h, 0, whole, 1, FROM_3)

    def forward(h, part):
        wait_for(h, (FROM_1, FROM_2)[part])
        gather_start(h, X, rows_of[part], Y, FROM_FAR)
        gather_start(h, Y, rows_of[2 + part], X, FROM_FAR)

    def share_near(h):
        wait_for(h, FROM_3)
        gather_start(h, X, whole, 1, SIB_XY)
        gather_start(h, Y, whole, 1, SIB_XY)

    def share_far(h):
        wait_for(h, FROM_FAR)
        gather_start(h, 6, whole, 1, SIB_D)

    def block_of(h, flip):
        if h is None:
            return jnp.concatenate([block_of(i, flip) for i in range(halves)], axis=1)
        return feat_ref[:, lanes(h)] if flip == 0 else gathered[h, r ^ flip]

    def product(h, flips, dest, group=None):
        columns = []
        for flip in flips:
            base = (r ^ flip) * (blocks * row_blocks)
            line = 2 * (slots // LANES) + base // LANES
            spot = base % LANES + dest * blocks
            columns += [(line, spot + k * row_blocks) for k in range(blocks)]
        picks = range(blocks) if group is None else [group * (blocks // 2) + k for k in range(blocks // 2)]
        left = jnp.concatenate(
            [jnp.concatenate([merged[table[line, spot + b]] for line, spot in columns], axis=1)
             for b in picks], axis=0)
        right = jnp.concatenate([block_of(h, flip) for flip in flips], axis=0)
        return jnp.dot(left, right, preferred_element_type=jnp.float32)

    def half_of(g):
        return pl.ds(pl.multiple_of(g * half_rows, half_rows), half_rows)

    def add_pair(h, flips, low, count):
        @pl.loop(low, low + count)
        def _(i):
            dest = jnp.where(i == 0, dests[0], dests[1])
            if flips[0] == 0:
                acc[h, i] = product(h, flips, dest)
            else:
                acc[h, i] += product(h, flips, dest)

    def piece(q, pieces):
        size = seg // pieces
        return pl.ds(pl.multiple_of(q * size, size), size)

    def sum_copy(src, dst, recv, row, col):
        return pltpu.make_async_remote_copy(
            src_ref=src, dst_ref=dst, send_sem=sent, recv_sem=recv,
            device_id=(row, col), device_id_type=MESH)

    def relay_copy(h, i, q):
        rows = piece(q, PIECES[h])
        return sum_copy(send.at[h, i, rows, :], relayed.at[h, i, rows, :],
                        relay_sem.at[2 * sum(PIECES[:h]) + i * PIECES[h] + q], r, near)

    def far_copy(h, i, q):
        rows = piece(q, PIECES[h])
        return sum_copy(send.at[h, i, rows, :], far.at[h, rows, :],
                        far_sem.at[0 if h == 0 else q + 1], r, dests[i])

    def near_copy(h, q):
        rows = piece(q, NEAR[h])
        return sum_copy(send_near.at[h, rows, :], near_in.at[h, rows, :],
                        near_sem.at[0 if h == 0 else q + 1], r, near)

    def last_pair(h, i):
        each = PIECES[h] // 2

        @pl.loop(0, 2)
        def _(g):
            rows = half_of(g)
            total = acc[h, i, rows, :] + product(h, (6, 7), dests[i], g)
            acc[h, i, rows, :] = total

            @pl.when(outer)
            def _():
                send[h, i, rows, :] = total.astype(send.dtype)
                for k in range(each):
                    relay_copy(h, i, g * each + k).start()

    def relay_sum(h, i, q):
        @pl.when(jnp.logical_not(outer))
        def _():
            rows = piece(q, PIECES[h])
            relay_copy(h, i, q).wait_recv()
            total = acc[h, i, rows, :] + relayed[h, i, rows, :].astype(jnp.float32)
            send[h, i, rows, :] = total.astype(send.dtype)
            far_copy(h, i, q).start()

    def tell_outer():
        @pl.when(jnp.logical_not(outer))
        def _():
            for col in (near, c ^ 2):
                pl.semaphore_signal(inner_ready, inc=1, device_id=(r, col), device_id_type=MESH)

    def hear_inner():
        @pl.when(outer)
        def _():
            pl.semaphore_wait(inner_ready, 2)

    def near_product(h, trips):
        @pl.loop(0, trips)
        def _(g):
            rows = half_of(g)
            send_near[h, rows, :] = product(h, range(n_row), near, g).astype(send_near.dtype)

    def near_segment(mine):
        near_product(1, jnp.where(mine, 2, 0))

        @pl.when(mine)
        def _():
            for q in range(NEAR[1]):
                near_copy(1, q).start()

    def near_first(mine, pieces):
        near_product(0, jnp.where(mine, 2, 0))

        @pl.when(mine)
        def _():
            for q in range(pieces):
                near_copy(0, q).start()

    def when(mine, *runs):
        @pl.when(mine)
        def _():
            for run, *args in runs:
                run(*args)

    def forwards(mine):
        @pl.when(mine)
        def _():
            forward(1, 0)
            forward(1, 1)

    def near_rest():
        @pl.when(outer)
        def _():
            near_copy(0, 1).start()

    def own_segment():
        @pl.loop(0, 2)
        def _(g):
            own[half_of(g), :] = product(None, range(n_row), c, g)

    def finish():
        sum_copy(far.at[0], far.at[0], far_sem.at[0], r, near).wait_recv()
        sum_copy(near_in.at[0], near_in.at[0], near_sem.at[0], r, near).wait_recv()
        pieces = NEAR[1]
        for q in range(pieces):
            rows = piece(q, pieces)
            far_copy(1, 0, q).wait_recv()
            near_copy(1, q).wait_recv()
            divisor = degree_col[rows, :]
            mean = jnp.concatenate(
                [((own[rows, lanes(h)] + far[h, rows, :].astype(jnp.float32)
                   + near_in[h, rows, :].astype(jnp.float32)) / divisor).astype(jnp.bfloat16)
                 for h in range(halves)], axis=1)
            mixed = hidden[rows, :] + jnp.dot(
                mean, proj_ref[width:, :], preferred_element_type=jnp.float32)
            out_ref[rows, :] = jnp.maximum(mixed, 0.0).astype(out_ref.dtype)

    def tables():
        fetch(0).wait()
        merged[slots] = jnp.zeros((tile, tile), merged.dtype)
        slot_tables(place_ref, count_ref[0], table_v, row_blocks, positions)

    table_copy = pltpu.make_async_copy(table_v, table, table_sem)

    def wait_loads():
        table_copy.wait()
        pltpu.make_async_copy(tiles_ref, stage, tile_sem).wait()

    def merge_slots(low, high, running):
        for part in range(slots // LANES):
            def merge(i, running, part=part):
                keep = table[slots // LANES + part, i].astype(jnp.float32)
                kept = jnp.broadcast_to(keep, (16, tile)).astype(running.dtype)
                kept = jnp.concatenate([kept] * (tile // 16), axis=0)
                running = stage[table[part, i]] + running * kept
                merged[part * LANES + i] = running
                return running
            begin, end = max(low - part * LANES, 0), min(high - part * LANES, LANES)
            if begin < end:
                running = lax.fori_loop(begin, end, merge, running, unroll=UNROLL)
        return running

    def prepare():
        for h in range(1, halves):
            fetch_features(h, whole).wait()
        for i in range(1, len(inputs)):
            fetch(i).wait()
        hidden[...] = jnp.dot(
            feat_ref[...], proj_ref[:width, :], preferred_element_type=jnp.float32) + bias_ref[...]
        for b in range(seg // LANES):
            one = degree_ref[b:b + 1, :].astype(jnp.float32)
            degree_col[b * LANES:(b + 1) * LANES, :] = jnp.transpose(jnp.broadcast_to(one, (LANES, LANES)))

    def drain():
        tiles_sent = halves * 10 * seg * LANES // (tile * tile)
        sum_copy(stage.at[pl.ds(0, tiles_sent)], stage.at[pl.ds(0, tiles_sent)],
                 near_sem.at[0], r, near).wait_send()

    def step(name, run, *args):
        with jax.named_scope(name):
            return run(*args)

    early = slots // 4
    inner = jnp.logical_not(outer)
    step("w_feat", fetch_features(0, whole).wait)
    step("barrier", pl.semaphore_wait, barrier, jnp.where(outer, 3, 6))
    step("own0", gather_own, 0)
    gather_sibling(0)
    tell_outer()
    step("tables", tables)
    table_copy.start()
    step("prepare", prepare)
    step("loads", wait_loads)
    step("forward0a", forward, 0, 0)
    running = step("merge0", merge_slots, 0, early, jnp.zeros((tile, tile), merged.dtype))
    step("forward0b", forward, 0, 1)
    step("own1i", when, inner, (gather_own, 1), (gather_sibling, 1))
    step("merge1", merge_slots, early, slots, running)
    step("share_near0", share_near, 0)
    step("pair0a0", add_pair, 0, (0, 1), 0, one)
    step("pair0a1", add_pair, 0, (0, 1), 1, one)
    step("share_far0", share_far, 0)
    step("own1o", when, outer, (gather_own, 1))
    step("w_x0", wait_for, 0, SIB_XY)
    step("pair0x0", add_pair, 0, (2, 3), 0, one)
    step("pair0y0", add_pair, 0, (4, 5), 0, one)
    step("w_d0", wait_for, 0, SIB_D)
    step("near_seg0i", near_first, inner, NEAR[0])
    step("forward1i", forwards, inner)
    step("share_near1i", when, inner, (share_near, 1))
    hear_inner()
    step("last00", last_pair, 0, 0)
    when(outer, (gather_sibling, 1))
    step("pair0x1", add_pair, 0, (2, 3), 1, one)
    step("pair0y1", add_pair, 0, (4, 5), 1, one)
    step("last01", last_pair, 0, 1)
    step("forward1o", forwards, outer)
    step("near_seg0o", near_first, outer, 1)
    step("share_near1o", when, outer, (share_near, 1))
    step("relay000", relay_sum, 0, 0, 0)
    step("pair1a", add_pair, 1, (0, 1), 0, 2)
    step("w_x1", wait_for, 1, SIB_XY)
    step("pair1x", add_pair, 1, (2, 3), 0, 2)
    step("share_far1", share_far, 1)
    step("relay001", relay_sum, 0, 0, 1)
    step("pair1y", add_pair, 1, (4, 5), 0, 2)
    step("relay010", relay_sum, 0, 1, 0)
    step("w_d1", wait_for, 1, SIB_D)
    step("near_seg1i", near_segment, jnp.logical_not(outer))
    step("relay011", relay_sum, 0, 1, 1)
    step("last10", last_pair, 1, 0)
    step("last11", last_pair, 1, 1)
    near_rest()
    step("near_seg1o", near_segment, outer)
    for i in range(2):
        for q in range(PIECES[1]):
            step(f"relay1{i}{q}", relay_sum, 1, i, q)
    step("own_seg", own_segment)
    step("finish", finish)
    step("drain", drain)


def local_fused(n_row, n_col, features, in_degree, tile_index, tile_count, adjacency_tiles, projection, out_bias):
    seg, width = features.shape
    slots, tile, _ = adjacency_tiles.shape
    halves = width // LANES
    positions = (seg * n_col // tile) * (seg * n_row // tile)
    lines = 2 * (slots // LANES) + positions // LANES
    hbm = pl.BlockSpec(memory_space=pltpu.HBM)
    args = [features, tile_index.T, tile_count, adjacency_tiles,
            in_degree.reshape(seg // LANES, LANES), projection, out_bias[None, :]]
    specs = [hbm] * len(args)
    specs[2] = pl.BlockSpec(memory_space=pltpu.SMEM)
    args = [a if i == 2 else pltpu.with_memory_space_constraint(a, pltpu.HBM) for i, a in enumerate(args)]
    return pl.pallas_call(
        fused_kernel,
        out_shape=jax.ShapeDtypeStruct((seg, projection.shape[1]), jnp.bfloat16),
        in_specs=specs,
        out_specs=pl.BlockSpec(memory_space=pltpu.VMEM),
        scratch_shapes=[
            pltpu.VMEM(features.shape, features.dtype),
            pltpu.VMEM((2, slots), jnp.int32),
            pltpu.VMEM((seg // LANES, LANES), jnp.int32),
            pltpu.VMEM(projection.shape, projection.dtype),
            pltpu.VMEM((1, projection.shape[1]), jnp.float32),
            pltpu.VMEM((slots, tile, tile), jnp.bfloat16),
            pltpu.VMEM((slots + 1, tile, tile), jnp.bfloat16),
            pltpu.VMEM((lines, LANES), jnp.int32),
            pltpu.SMEM((lines, LANES), jnp.int32),
            pltpu.VMEM((halves, n_row, seg, LANES), jnp.bfloat16),
            pltpu.VMEM((halves, 2, seg, LANES), jnp.float32),
            pltpu.VMEM((seg, width), jnp.float32),
            pltpu.VMEM((seg, projection.shape[1]), jnp.float32),
            pltpu.VMEM((seg, LANES), jnp.float32),
            pltpu.VMEM((halves, 2, seg, LANES), jnp.bfloat16),
            pltpu.VMEM((halves, seg, LANES), jnp.bfloat16),
            pltpu.VMEM((halves, 2, seg, LANES), jnp.bfloat16),
            pltpu.VMEM((halves, seg, LANES), jnp.bfloat16),
            pltpu.VMEM((halves, seg, LANES), jnp.bfloat16),
            pltpu.SemaphoreType.DMA((halves + len(args) - 3,)),
            pltpu.SemaphoreType.DMA,
            pltpu.SemaphoreType.DMA,
            pltpu.SemaphoreType.DMA,
            pltpu.SemaphoreType.DMA((halves, ARRIVALS)),
            pltpu.SemaphoreType.DMA((2 * sum(PIECES),)),
            pltpu.SemaphoreType.DMA((1 + PIECES[1],)),
            pltpu.SemaphoreType.DMA((1 + NEAR[1],)),
            pltpu.SemaphoreType.REGULAR,
        ],
        compiler_params=pltpu.CompilerParams(
            collective_id=0, has_side_effects=True, vmem_limit_bytes=48 * 1024 * 1024),
    )(*args)


def solution(mesh):
    n_row, n_col = mesh.shape["row"], mesh.shape["col"]

    def local(features, in_degree, tile_index, tile_count, adjacency_tiles, projection, out_bias):
        seg, width = features.shape
        slots, tile, _ = adjacency_tiles.shape
        positions = (seg * n_col // LANES) * (seg * n_row // LANES)
        fits = (
            n_row == 8 and n_col == 4 and tile == LANES and slots <= 256 and slots % LANES == 0
            and 4 * slots * tile * tile <= MERGE_LIMIT
            and seg % (4 * LANES) == 0 and width == 2 * LANES and positions % LANES == 0
            and LANES % (positions // n_row) == 0)
        args = (features, in_degree, tile_index, tile_count, adjacency_tiles, projection, out_bias)
        return local_fused(n_row, n_col, *args) if fits else local_sparse(*args)

    return jax.shard_map(
        local,
        mesh=mesh,
        in_specs=(
            P(("row", "col"), None),
            P(("row", "col")),
            P(("row", "col"), None),
            P(("row", "col")),
            P(("row", "col"), None, None),
            P(),
            P(),
        ),
        out_specs=P(("row", "col"), None),
        check_vma=False,
    )
```
